128 devices in a mesh: band: 32 (over y, x_hi, z), grid: 4 (over x_lo, core).
Axes of the slice: x: 4 (x_hi: 2, x_lo: 2; x = x_hi * 2 + x_lo), y: 4, z: 4, core: 2. Of those that a mesh axis runs over, the one named last changes fastest.
Arguments:
- orbitals: float32 [96, 64, 4096], P('band', 'grid'), may hold values from -6 to 6
- pair_mask: int32 [96, 96], replicated, may hold values from 0 to 1, as said below
Outputs:
- exchange_term: float32 [96, 64, 4096], P('band', 'grid')
The draws below stay inside these ranges and needn't reach their ends.
Inputs may be any that keep to these rules, and one draw needn't show every extreme that they name: pair_mask is symmetric; entries outside the candidate pairs of every block (and their transposes) are 0; each block has at most 12 candidate pairs with mask 1, and some block has exactly 12.
All inputs are finite; a program needn't handle non-finite values.
Results may differ from the reference program's by a relative error of at most 0.00027.
Values sent between devices are 32-bit elements; how exact they have to be, the bound alone decides.
A program may use at most 64 MiB of HBM per device.

```python
import math
import jax
import jax.numpy as jnp
import numpy as np
from jax import lax

NG = 64
ORB_DEV = 3
REACH = 2
NORB = 96
NCAND = 24
CAP = 12


def pair_table_drawn():
    entries = []
    for distance in range(REACH + 1):
        for leading_orbital in range(ORB_DEV):
            for second_orb in range(ORB_DEV):
                if distance > 0 or leading_orbital <= second_orb:
                    entries.append((leading_orbital, distance, second_orb))
    return np.array(entries, dtype=np.int32)


def draw_orbitals(key, part):
    full_shape = (NORB, NG, NG * NG)
    values_out = jax.random.normal(key, full_shape, jnp.float32)
    return jnp.clip(values_out, -6.0, 6.0)


def draw_pair_mask(key, part):
    pair_list = pair_table_drawn()
    groups = NORB // ORB_DEV
    key_counts, key_full, key_scores = jax.random.split(jax.random.fold_in(key, 17), 3)
    counts = jax.random.randint(key_counts, (groups,), 1, CAP + 1)
    full_group = jax.random.randint(key_full, (), 0, groups)
    counts = jnp.where(jnp.arange(groups, dtype=jnp.int32) == full_group, CAP, counts)
    scores = jax.random.randint(key_scores, (groups, NCAND), 0, 1 << 20) * NCAND + jnp.arange(NCAND, dtype=jnp.int32)[None, :]
    ranks = jnp.argsort(jnp.argsort(scores, axis=1), axis=1)
    live_flags = (ranks < counts[:, None]).astype(jnp.int32)
    group_ids = jnp.arange(groups, dtype=jnp.int32)[:, None]
    row_ids = group_ids * ORB_DEV + jnp.asarray(pair_list[:, 0])[None, :]
    col_ids = (group_ids + jnp.asarray(pair_list[:, 1])[None, :]) % groups * ORB_DEV + jnp.asarray(pair_list[:, 2])[None, :]
    mask_out = jnp.zeros((NORB, NORB), jnp.int32)
    mask_out = mask_out.at[row_ids.reshape(-1), col_ids.reshape(-1)].set(live_flags.reshape(-1))
    mask_out = mask_out.at[col_ids.reshape(-1), row_ids.reshape(-1)].set(live_flags.reshape(-1))
    return mask_out


def setup_inputs(seed: int = 0) -> dict:
    key_list = jax.random.split(jax.random.key(seed), 3)
    return {
        "orbitals": draw_orbitals(jax.random.fold_in(key_list[2], 71), 0),
        "pair_mask": draw_pair_mask(jax.random.fold_in(key_list[2], 71), 0),
    }


MIXING = 0.25
BOX_LENGTH = 16.0


def pair_table():
    entries = []
    for distance in range(REACH + 1):
        for leading_orbital in range(ORB_DEV):
            for second_orb in range(ORB_DEV):
                if distance > 0 or leading_orbital <= second_orb:
                    entries.append((leading_orbital, distance, second_orb))
    return np.array(entries, dtype=np.int32)


def poisson_green_kernel():
    positions = jnp.arange(NG, dtype=jnp.int32)
    signed_waves = jnp.where(positions < NG // 2, positions, positions - NG)
    squared = (signed_waves[:, None, None] ** 2 + signed_waves[None, :, None] ** 2
               + signed_waves[None, None, :] ** 2)
    safe_values = jnp.maximum(squared, 1).astype(jnp.float32)
    return jnp.where(squared > 0, jnp.float32(BOX_LENGTH * BOX_LENGTH / math.pi) / safe_values,
                     jnp.float32(0.0))


def reference(orbitals, pair_mask):
    groups = NORB // ORB_DEV
    pair_list = pair_table()
    band_ids = np.arange(groups, dtype=np.int32)[:, None]
    row_ids = (band_ids * ORB_DEV + pair_list[None, :, 0]).reshape(-1).astype(np.int32)
    col_ids = (((band_ids + pair_list[None, :, 1]) % groups) * ORB_DEV
               + pair_list[None, :, 2]).reshape(-1).astype(np.int32)
    weights = pair_mask[jnp.asarray(row_ids), jnp.asarray(col_ids)].astype(jnp.float32)
    cross_flags = jnp.asarray((row_ids != col_ids).astype(np.float32)).astype(jnp.float32)
    cubes = orbitals.reshape(NORB, NG, NG, NG)
    kernel = poisson_green_kernel()

    def one_pair(totals, pair_input):
        row_id, col_id, weight, cross_flag = pair_input
        first_cube = cubes[row_id]
        second_cube = cubes[col_id]
        potential = jnp.real(jnp.fft.ifftn(jnp.fft.fftn(first_cube * second_cube) * kernel))
        totals = totals.at[row_id].add(weight * potential * second_cube)
        totals = totals.at[col_id].add(weight * cross_flag * potential * first_cube)
        return totals, None

    totals, discarded_value = lax.scan(one_pair, jnp.zeros((NORB, NG, NG, NG), jnp.float32),
                              (jnp.asarray(row_ids).astype(jnp.int32), jnp.asarray(col_ids).astype(jnp.int32),
                               weights, cross_flags))
    return (-MIXING * totals).reshape(NORB, NG, NG * NG)
```

```python
import functools

import jax
import jax.numpy as jnp
import numpy as np
from jax import lax
from jax.experimental import pallas as pl
from jax.experimental.pallas import tpu as pltpu
from jax.sharding import PartitionSpec as P

NG = 64
ORB = 3
MIXING = 0.25
BOX = 16.0
NC = 4
CY = 32 // NC
CL = CY * 128
PITCH = 72
MESH = pl.DeviceIdType.MESH
F32 = jnp.float32
BF16 = jnp.bfloat16


def hi_lo(values):
    hi = values.astype(BF16)
    return hi, (values - hi.astype(F32)).astype(BF16)


def host_hi_lo(values):
    hi = values.astype(np.float32).astype(BF16)
    return hi, (values - hi.astype(np.float64)).astype(np.float32).astype(BF16)


def tables():
    n = np.arange(NG)
    angle = 2.0 * np.pi * ((n[:, None] * n[None, :]) % NG) / NG
    h = (np.cos(angle) + np.sin(angle)) / 8.0
    hh, hl = host_hi_lo(h)
    ax = np.concatenate([hh, hl, hh], axis=1)
    bh, bl = host_hi_lo(np.kron(np.eye(2), h))
    wz = np.block([[bh, bl], [bh, np.zeros_like(bl)]])
    order = np.array([2 * (c % 32) + c // 32 for c in range(NG)])
    fh, fl = host_hi_lo(h[:, order])
    ay = np.concatenate([fh, fl, fh], axis=1)
    gh, gl = host_hi_lo(h[order, :])
    ai = np.concatenate([gh, gl, gh], axis=1)
    return ax, wz, ay, ai


def candidates():
    rows = []
    for first, second, same, kind in (
        (0, 2, False, 0),
        (1, 2, False, 1),
        (0, 1, False, 2),
        (1, 1, True, 3),
        (0, 0, True, 4),
        (2, 2, True, 5),
    ):
        for a in range(ORB):
            for b in range(ORB):
                if not same or a <= b:
                    rows.append((first, a, second, b, kind, 1))
    table = np.zeros((8, 128), np.int32)
    for c, row in enumerate(rows):
        table[:6, c] = row
    kind = np.where(table[5] > 0, table[4], -1)
    before = np.arange(128)[:, None] < np.arange(128)[None, :]
    same_kind = before & (kind[:, None] == kind[None, :])
    return table, same_kind.astype(np.float32), before.astype(np.float32)


def plan_kernel(slots, capacity, mask_ref, cand_ref, same_ref, before_ref, tab_ref, coef_ref):
    norb = mask_ref.shape[0]
    groups = norb // ORB
    group = lax.axis_index("band")
    m = mask_ref[...].astype(F32)
    rows = lax.broadcasted_iota(jnp.int32, (norb, norb), 0)
    cols = lax.broadcasted_iota(jnp.int32, (norb, norb), 1)
    brow = (rows * 21846) >> 16
    bcol = (cols * 21846) >> 16
    sep = jnp.where(bcol >= brow, bcol - brow, bcol - brow + groups)

    def row_sum(keep):
        return jnp.sum(jnp.where(keep, m, 0.0), axis=1, keepdims=True)

    r0 = row_sum((sep == 0) & (rows <= cols))
    r1 = row_sum(sep == 1)
    r2 = row_sum(sep == 2)
    gb = (lax.broadcasted_iota(jnp.int32, (norb, 128), 0) * 21846) >> 16
    lane = lax.broadcasted_iota(jnp.int32, (norb, 128), 1)
    nxt = jnp.where(gb == groups - 1, 0, gb + 1)
    prv = jnp.where(gb == 0, groups - 1, gb - 1)

    def to_lanes(values, place):
        return jnp.sum(jnp.where(place == lane, values, 0.0), axis=0, keepdims=True)

    n0 = to_lanes(r0, gb)
    n0_next = to_lanes(r0, prv)
    n1 = to_lanes(r1, gb)
    load = to_lanes(r2, nxt) + n1 + n0
    sub = lax.broadcasted_iota(jnp.int32, (128, 128), 0)
    lan = lax.broadcasted_iota(jnp.int32, (128, 128), 1)
    eye = sub == lan

    def to_rows(values):
        return jnp.sum(jnp.where(eye, values, 0.0), axis=1, keepdims=True)

    excess = jnp.where(sub < groups, to_rows(load) - capacity, 0.0)
    prefix = jnp.sum(jnp.where(sub <= lan, excess, 0.0), axis=0, keepdims=True)
    total = jnp.sum(excess, axis=0, keepdims=True)
    low = -jnp.floor(n0_next * 0.5)
    path = to_rows(prefix) - prefix + jnp.where(sub < lan, total, 0.0) + low
    flow = jnp.max(jnp.where(lan < groups, path, -1e9), axis=1, keepdims=True)

    left = jnp.where(group == 0, groups - 1, group - 1)
    right = jnp.where(group == groups - 1, 0, group + 1)
    sub1 = lax.broadcasted_iota(jnp.int32, (128, 1), 0)
    lan1 = lax.broadcasted_iota(jnp.int32, (1, 128), 1)

    def at_row(values, index):
        return jnp.sum(jnp.where(sub1 == index, values, 0.0), axis=0, keepdims=True)

    def at_lane(values, index):
        return jnp.sum(jnp.where(lan1 == index, values, 0.0), axis=1, keepdims=True)

    f_here, f_left = at_row(flow, group), at_row(flow, left)
    n1_here, n1_left = at_lane(n1, group), at_lane(n1, left)
    n0_here, n0_right = at_lane(n0, group), at_lane(n0, right)

    cand = cand_ref[...]

    def orbital_of(block, inner):
        b = group + block - 1
        b = jnp.where(b < 0, b + groups, jnp.where(b >= groups, b - groups, b))
        return b * ORB + inner

    row_id = orbital_of(cand[0:1], cand[1:2])
    col_id = orbital_of(cand[2:3], cand[3:4])
    kind = cand[4:5]
    valid = cand[5:6] > 0
    orb = lax.broadcasted_iota(jnp.int32, (norb, 128), 0)
    col_hot = (orb == col_id).astype(F32)
    picked = jnp.dot(m, col_hot, preferred_element_type=F32)
    live = jnp.sum(jnp.where(orb == row_id, picked, 0.0), axis=0, keepdims=True)
    live = jnp.where(valid, live, 0.0)
    rank = jnp.dot(
        jnp.broadcast_to(live, (8, 128)), same_ref[...], preferred_element_type=F32
    )[0:1]
    big = 1e9
    x1 = jnp.minimum(jnp.maximum(f_here, 0.0), n1_here)
    y1 = jnp.minimum(jnp.maximum(f_left, 0.0), n1_left)
    b0 = jnp.maximum(f_here - n1_here, 0.0)
    a0 = jnp.maximum(-f_left, 0.0)
    low_rank = jnp.where(
        kind == 1,
        x1,
        jnp.where(kind == 3, b0, jnp.where(kind == 5, n0_right - jnp.maximum(-f_here, 0.0), 0.0)),
    )
    high_rank = jnp.where(
        kind == 2,
        y1,
        jnp.where(
            kind == 3, n0_here - a0, jnp.where(kind == 4, jnp.maximum(f_left - n1_left, 0.0), big)
        ),
    )
    active = jnp.where((rank >= low_rank) & (rank < high_rank), live, 0.0)
    place = jnp.dot(
        jnp.broadcast_to(active, (8, 128)), before_ref[...], preferred_element_type=F32
    )[0:1]
    slot = lax.broadcasted_iota(jnp.int32, (slots, 128), 0).astype(F32)
    hot = jnp.where(place == slot, active, 0.0)
    first = (cand[0:1] * ORB + cand[1:2]).astype(F32)
    second = (cand[2:3] * ORB + cand[3:4]).astype(F32)
    i_of = jnp.sum(hot * first, axis=1, keepdims=True)
    j_of = jnp.sum(hot * second, axis=1, keepdims=True)
    w_of = jnp.sum(hot, axis=1, keepdims=True)
    lane_s = lax.broadcasted_iota(jnp.int32, (slots, 128), 1)
    tab_ref[...] = jnp.where(lane_s == 0, i_of, jnp.where(lane_s == 1, j_of, 0.0)).astype(jnp.int32)
    w_cross = jnp.where(i_of == j_of, 0.0, w_of)
    for q in range(3 * ORB):
        coef_ref[0, q] = jnp.broadcast_to(jnp.where(i_of == q, w_of, 0.0), (slots, 128))
        coef_ref[1, q] = jnp.broadcast_to(jnp.where(j_of == q, w_cross, 0.0), (slots, 128))


def plan(slots, capacity, pair_mask):
    table, same_kind, before = candidates()
    vmem = pl.BlockSpec(memory_space=pltpu.VMEM)
    return pl.pallas_call(
        functools.partial(plan_kernel, slots, float(capacity)),
        out_shape=(
            jax.ShapeDtypeStruct((slots, 128), jnp.int32),
            jax.ShapeDtypeStruct((2, 3 * ORB, slots, 128), F32),
        ),
        in_specs=[vmem] * 4,
        out_specs=(vmem, vmem),
        name="plan",
    )(pair_mask, jnp.asarray(table), jnp.asarray(same_kind), jnp.asarray(before))


def split_sum(low_mask, tall):
    half = tall.shape[0] // 2
    outs = []
    for t in range(tall.shape[1] // 128):
        top = tall[:half, t * 128 : (t + 1) * 128]
        bot = tall[half:, t * 128 : (t + 1) * 128]
        outs.append(
            jnp.where(low_mask, top, bot) + pltpu.roll(jnp.where(low_mask, bot, top), 64, 1)
        )
    return outs


def mega_kernel(rounds, *refs):
    (tab, coef, ax_ref, wz_ref, ay_ref, ai_ref, orb_hbm, out_ref) = refs[:8]
    orbs = refs[8 : 8 + NC]
    sums = refs[8 + NC : 8 + 2 * NC]
    back = refs[8 + 2 * NC : 8 + 3 * NC]
    (rho, cube, work, vout, vrecv, ktab) = refs[8 + 3 * NC : 14 + 3 * NC]
    (lsem, z1s, z1r, x1s, x1r, x2s, x2r, z2s, z2r) = refs[14 + 3 * NC :]

    groups = lax.axis_size("band")
    band = lax.axis_index("band")
    me = lax.axis_index("grid")
    left = lax.rem(band + groups - 1, groups)
    right = lax.rem(band + 1, groups)
    peers = {
        0: me,
        1: me + 1 - 2 * lax.rem(me, 2),
        2: lax.rem(me + 2, 4),
        3: 3 - me,
    }

    def local_copy(c):
        return pltpu.make_async_copy(
            orb_hbm.at[:, :, pl.ds(c * CL, CL)], orbs[c].at[pl.ds(ORB, ORB)], lsem.at[c]
        )

    for c in range(NC):
        local_copy(c).start()

    barrier = pltpu.get_barrier_semaphore()
    for target in (left, right):
        pl.semaphore_signal(barrier, inc=1, device_id=(target, me), device_id_type=MESH)
    for k in (1, 2, 3):
        pl.semaphore_signal(barrier, inc=1, device_id=(band, peers[k]), device_id_type=MESH)
    pl.semaphore_wait(barrier, 5)

    def z1(side, c):
        return pltpu.make_async_remote_copy(
            src_ref=orbs[c].at[pl.ds(ORB, ORB)],
            dst_ref=orbs[c].at[pl.ds(2 * ORB if side == 0 else 0, ORB)],
            send_sem=z1s.at[side, c],
            recv_sem=z1r.at[side, c],
            device_id=(left if side == 0 else right, me),
            device_id_type=MESH,
        )

    for c in range(NC):
        local_copy(c).wait()
        z1(0, c).start()
        z1(1, c).start()

    low_mask = lax.broadcasted_iota(jnp.int32, (32, 128), 1) < 64

    def signed(k):
        return jnp.where(k < NG // 2, k, k - NG)

    lane = lax.broadcasted_iota(jnp.int32, (32, 128), 1)
    sub = lax.broadcasted_iota(jnp.int32, (32, 128), 0)
    fy = signed(sub + jnp.where(low_mask, 0, 32))
    fz = signed(jnp.where(low_mask, lane, lane - 64))
    flat = fy * fy + fz * fz

    def fill(kx, carry):
        fx = signed(kx)
        squared = flat + fx * fx
        safe = jnp.maximum(squared, 1).astype(F32)
        ktab[pl.ds(pl.multiple_of(kx * 32, 32), 32), :] = jnp.where(
            squared > 0, (BOX * BOX / np.pi) / safe, 0.0
        )
        return carry

    lax.fori_loop(0, NG, fill, 0)

    def x1(k, r, c):
        return pltpu.make_async_remote_copy(
            src_ref=rho.at[k - 1, r, pl.ds(c * CY, CY)],
            dst_ref=cube.at[r, pl.ds(c * CY, CY), me],
            send_sem=x1s.at[k - 1, r, c],
            recv_sem=x1r.at[k - 1, r, c],
            device_id=(band, peers[k]),
            device_id_type=MESH,
        )

    def x2(k, r, c):
        return pltpu.make_async_remote_copy(
            src_ref=vout.at[r, pl.ds(c * CY, CY), peers[k]],
            dst_ref=vrecv.at[k - 1, r, pl.ds(c * CY, CY)],
            send_sem=x2s.at[k - 1, r, c],
            recv_sem=x2r.at[k - 1, r, c],
            device_id=(band, peers[k]),
            device_id_type=MESH,
        )

    def z2(side, c):
        return pltpu.make_async_remote_copy(
            src_ref=sums[c].at[pl.ds(0 if side == 0 else 2 * ORB, ORB)],
            dst_ref=back[c].at[1 if side == 0 else 0],
            send_sem=z2s.at[side, c],
            recv_sem=z2r.at[side, c],
            device_id=(left if side == 0 else right, me),
            device_id_type=MESH,
        )

    def lanes(y):
        return pl.ds(pl.multiple_of(y * 128, 128), 128)

    for c in range(NC):
        z1(0, c).wait_recv()
        z1(1, c).wait_recv()
        for r in range(rounds):
            ids = {}
            for k in (2, 3, 1, 0):
                slot = r * 4 + peers[k]
                ids[k] = (tab[slot, 0], tab[slot, 1])

            def densities(y, carry, c=c, r=r, ids=ids):
                for k in (2, 3, 1, 0):
                    i, j = ids[k]
                    value = orbs[c][i, :, lanes(y)] * orbs[c][j, :, lanes(y)]
                    if k == 0:
                        cube[r, c * CY + y, me] = value
                    else:
                        rho[k - 1, r, c * CY + y] = value
                return carry

            lax.fori_loop(0, CY, densities, 0)
            for k in (2, 3, 1):
                x1(k, r, c).start()

    ax = ax_ref[...]
    wz = wz_ref[...]

    def along_z(tiles):
        stacked = jnp.concatenate(tiles, axis=0)
        hi, lo = hi_lo(stacked)
        wide = jnp.dot(jnp.concatenate([hi, lo], axis=1), wz, preferred_element_type=F32)
        both = wide[:, :128] + wide[:, 128:]
        return [both[t * NG : (t + 1) * NG] for t in range(len(tiles))]

    def along_x(tiles):
        outs = []
        for t in range(0, len(tiles), 2):
            hi, lo = hi_lo(jnp.concatenate([tiles[t], tiles[t + 1]], axis=1))
            wide = jnp.dot(ax, jnp.concatenate([hi, hi, lo], axis=0), preferred_element_type=F32)
            outs += [wide[:, :128], wide[:, 128:]]
        return outs

    def work_rows(r, y):
        return pl.ds(pl.multiple_of((r * 32 + y) * PITCH, 8), NG)

    def forward(step, carry):
        c, r = step // rounds, lax.rem(step, rounds)
        for k in (1, 2, 3):
            x1(k, r, c).wait_recv()
        tiles = [cube[r, c * CY + t].reshape(NG, 128) for t in range(CY)]
        tiles = along_z(along_x(tiles))
        for t in range(CY):
            work[work_rows(r, c * CY + t), :] = tiles[t]
        return carry

    lax.fori_loop(0, NC * rounds, forward, 0)

    def spread(tiles):
        hi, lo = hi_lo(jnp.concatenate(tiles, axis=1))
        mask = lax.rem(lax.broadcasted_iota(jnp.int32, hi.shape, 1), 128) < 64
        zero = jnp.zeros_like(hi)
        h0, h1 = jnp.where(mask, hi, zero), jnp.where(mask, zero, hi)
        l0, l1 = jnp.where(mask, lo, zero), jnp.where(mask, zero, lo)
        return jnp.concatenate([h0, h1, h0, h1, l0, l1], axis=0)

    ay = ay_ref[...]
    ai = ai_ref[...]
    KX = 8

    def middle(step, carry):
        r, g = step // (NG // KX), lax.rem(step, NG // KX)
        base = r * (32 * PITCH) + g * KX
        for t in range(0, KX, 2):
            tiles = [work[pl.ds(base + t + u, 32, stride=PITCH), :] for u in range(2)]
            tiles = split_sum(low_mask, jnp.dot(ay, spread(tiles), preferred_element_type=F32))
            tiles = [
                tiles[u] * ktab[pl.ds(pl.multiple_of((g * KX + t + u) * 32, 32), 32), :]
                for u in range(2)
            ]
            tiles = split_sum(low_mask, jnp.dot(ai, spread(tiles), preferred_element_type=F32))
            for u in range(2):
                work[pl.ds(base + t + u, 32, stride=PITCH), :] = tiles[u]
        return carry

    lax.fori_loop(0, rounds * (NG // KX), middle, 0)

    def inverse(step, carry):
        c, r = step // rounds, lax.rem(step, rounds)
        tiles = [work[work_rows(r, c * CY + t), :] for t in range(CY)]
        tiles = along_x(along_z(tiles))
        for t in range(CY):
            vout[r, c * CY + t] = tiles[t].reshape(4, 16, 128)
        for k in (2, 3, 1):
            x2(k, r, c).start()
        return carry

    lax.fori_loop(0, NC * rounds, inverse, 0)

    for c in range(NC):
        for r in range(rounds):
            for k in (1, 2, 3):
                x2(k, r, c).wait_recv()
        ids = {}
        for r in range(rounds):
            for k in range(4):
                slot = r * 4 + peers[k]
                ids[r, k] = (slot, tab[slot, 0], tab[slot, 1])

        def accumulate(y, carry, c=c, ids=ids):
            totals = [jnp.zeros((16, 128), F32) for _ in range(3 * ORB)]
            for r in range(rounds):
                for k in range(4):
                    slot, i, j = ids[r, k]
                    if k == 0:
                        v = vout[r, c * CY + y, me]
                    else:
                        v = vrecv[k - 1, r, c * CY + y]
                    on_i = v * orbs[c][j, :, lanes(y)]
                    on_j = v * orbs[c][i, :, lanes(y)]
                    for q in range(3 * ORB):
                        totals[q] = (
                            totals[q]
                            + coef[0, q, pl.ds(slot, 1), :] * on_i
                            + coef[1, q, pl.ds(slot, 1), :] * on_j
                        )
            for q in range(3 * ORB):
                sums[c][q, :, lanes(y)] = totals[q]
            return carry

        lax.fori_loop(0, CY, accumulate, 0)
        z2(0, c).start()
        z2(1, c).start()

    for c in range(NC):
        z2(0, c).wait_recv()
        z2(1, c).wait_recv()
        for a in range(ORB):
            out_ref[a, :, pl.ds(c * CL, CL)] = -MIXING * (
                sums[c][ORB + a] + (back[c][0, a] + back[c][1, a])
            )

    for c in range(NC):
        for side in range(2):
            z1(side, c).wait_send()
            z2(side, c).wait_send()

    def drain(step, carry):
        c, r = step // rounds, lax.rem(step, rounds)
        for k in (1, 2, 3):
            x1(k, r, c).wait_send()
            x2(k, r, c).wait_send()
        return carry

    lax.fori_loop(0, NC * rounds, drain, 0)


def mega(rounds, collective_id, tab, coef, orbitals):
    ax, wz, ay, ai = tables()
    vmem = pl.BlockSpec(memory_space=pltpu.VMEM)
    planes = orbitals.shape[1]
    dma = pltpu.SemaphoreType.DMA
    return pl.pallas_call(
        functools.partial(mega_kernel, rounds),
        out_shape=jax.ShapeDtypeStruct(orbitals.shape, F32),
        in_specs=[pl.BlockSpec(memory_space=pltpu.SMEM)]
        + [vmem] * 5
        + [pl.BlockSpec(memory_space=pl.ANY)],
        out_specs=vmem,
        scratch_shapes=[pltpu.VMEM((3 * ORB, planes, CL), F32) for _ in range(2 * NC)]
        + [pltpu.VMEM((2, ORB, planes, CL), F32) for _ in range(NC)]
        + [
            pltpu.VMEM((3, rounds, 32, planes, 128), F32),
            pltpu.VMEM((rounds, 32, 4, planes, 128), F32),
            pltpu.VMEM((rounds * 32 * PITCH, 128), F32),
            pltpu.VMEM((rounds, 32, 4, planes, 128), F32),
            pltpu.VMEM((3, rounds, 32, planes, 128), F32),
            pltpu.VMEM((NG * 32, 128), F32),
            dma((NC,)),
            dma((2, NC)),
            dma((2, NC)),
            dma((3, rounds, NC)),
            dma((3, rounds, NC)),
            dma((3, rounds, NC)),
            dma((3, rounds, NC)),
            dma((2, NC)),
            dma((2, NC)),
        ],
        compiler_params=pltpu.CompilerParams(
            collective_id=collective_id, has_side_effects=True, vmem_limit_bytes=56 * 1024 * 1024
        ),
        name="mega%d" % rounds,
    )(
        tab,
        coef,
        jnp.asarray(ax),
        jnp.asarray(wz),
        jnp.asarray(ay),
        jnp.asarray(ai),
        orbitals,
    )


def local(orbitals, pair_mask):
    tab, coef = plan(16, 12, pair_mask)
    return mega(3, 3, tab, coef, orbitals)


def solution(mesh):
    return jax.shard_map(
        local,
        mesh=mesh,
        in_specs=(P("band", "grid", None), P()),
        out_specs=P("band", "grid", None),
        check_vma=False,
    )
```

```python
import functools

import jax
import jax.numpy as jnp
import numpy as np
from jax import lax
from jax.experimental import pallas as pl
from jax.experimental.pallas import tpu as pltpu
from jax.sharding import PartitionSpec as P

NG = 64
ORB = 3
MIXING = 0.25
BOX = 16.0
NC = 4
CY = 32 // NC
CL = CY * 128
KX = 16
CLASSES = ((8, 12), (10, 12), (12, 12))
PITCH = 72
MESH = pl.DeviceIdType.MESH
F32 = jnp.float32
BF16 = jnp.bfloat16


def hi_lo(values):
    hi = values.astype(BF16)
    return hi, (values - hi.astype(F32)).astype(BF16)


def host_hi_lo(values):
    hi = values.astype(np.float32).astype(BF16)
    return hi, (values - hi.astype(np.float64)).astype(np.float32).astype(BF16)


def tables():
    n = np.arange(NG)
    angle = 2.0 * np.pi * ((n[:, None] * n[None, :]) % NG) / NG
    h = (np.cos(angle) + np.sin(angle)) / 8.0
    hh, hl = host_hi_lo(h)
    ax = np.concatenate([hh, hl, hh], axis=1)
    bh, bl = host_hi_lo(np.kron(np.eye(2), h))
    wz = np.block([[bh, bl], [bh, np.zeros_like(bl)]])
    fh, fl = host_hi_lo(np.concatenate([h[:, 0::2], h[:, 1::2]], axis=0))
    ay = np.concatenate([fh, fl, fh], axis=1)
    back = np.concatenate([h[0::2], h[1::2]], axis=0)
    gh, gl = host_hi_lo(np.concatenate([back[:, :32], back[:, 32:]], axis=0))
    ai = np.concatenate([gh, gl, gh], axis=1)
    return ax, wz, ay, ai


def candidates():
    rows = []
    for first, second, same, kind in (
        (0, 2, False, 0),
        (1, 2, False, 1),
        (0, 1, False, 2),
        (1, 1, True, 3),
        (0, 0, True, 4),
        (2, 2, True, 5),
    ):
        for a in range(ORB):
            for b in range(ORB):
                if not same or a <= b:
                    rows.append((first, a, second, b, kind, 1))
    table = np.zeros((8, 128), np.int32)
    for c, row in enumerate(rows):
        table[:6, c] = row
    kind = np.where(table[5] > 0, table[4], -1)
    before = np.arange(128)[:, None] < np.arange(128)[None, :]
    same_kind = before & (kind[:, None] == kind[None, :])
    return table, same_kind.astype(np.float32), before.astype(np.float32)


def plan_kernel(slots, classes, mask_ref, cand_ref, same_ref, before_ref, tab_ref, coef_ref, class_ref):
    norb = mask_ref.shape[0]
    groups = norb // ORB
    group = lax.axis_index("band")
    m = mask_ref[...].astype(F32)
    rows = lax.broadcasted_iota(jnp.int32, (norb, norb), 0)
    cols = lax.broadcasted_iota(jnp.int32, (norb, norb), 1)
    brow = (rows * 21846) >> 16
    bcol = (cols * 21846) >> 16
    sep = jnp.where(bcol >= brow, bcol - brow, bcol - brow + groups)

    def row_sum(keep):
        return jnp.sum(jnp.where(keep, m, 0.0), axis=1, keepdims=True)

    r0 = row_sum((sep == 0) & (rows <= cols))
    r1 = row_sum(sep == 1)
    r2 = row_sum(sep == 2)
    gb = (lax.broadcasted_iota(jnp.int32, (norb, 128), 0) * 21846) >> 16
    lane = lax.broadcasted_iota(jnp.int32, (norb, 128), 1)
    nxt = jnp.where(gb == groups - 1, 0, gb + 1)
    prv = jnp.where(gb == 0, groups - 1, gb - 1)

    def to_lanes(values, place):
        return jnp.sum(jnp.where(place == lane, values, 0.0), axis=0, keepdims=True)

    n0 = to_lanes(r0, gb)
    n0_next = to_lanes(r0, prv)
    n1 = to_lanes(r1, gb)
    load = to_lanes(r2, nxt) + n1 + n0
    sub = lax.broadcasted_iota(jnp.int32, (128, 128), 0)
    lan = lax.broadcasted_iota(jnp.int32, (128, 128), 1)
    eye = sub == lan

    def to_rows(values):
        return jnp.sum(jnp.where(eye, values, 0.0), axis=1, keepdims=True)

    low = -jnp.floor(n0_next * 0.5)
    high = to_rows(n1 + jnp.floor((n0 + 1.0) * 0.5))
    load_rows = to_rows(load)
    is_edge = lax.rem((sub + 1) // 2, 2) == 0
    choice, flow = None, None
    for index in reversed(range(len(classes))):
        edge, inner = classes[index]
        excess = load_rows - jnp.where(is_edge, float(edge), float(inner))
        excess = jnp.where(sub < groups, excess, 0.0)
        prefix = jnp.sum(jnp.where(sub <= lan, excess, 0.0), axis=0, keepdims=True)
        total = jnp.sum(excess, axis=0, keepdims=True)
        path = to_rows(prefix) - prefix + jnp.where(sub < lan, total, 0.0) + low
        need = jnp.max(jnp.where(lan < groups, path, -1e9), axis=1, keepdims=True)
        if choice is None:
            choice, flow = jnp.full((1, 1), float(index), F32), need
        else:
            over = jnp.where(sub[:, :1] < groups, need - high, -1e9)
            worst = jnp.maximum(jnp.max(over, axis=0, keepdims=True), total[:, :1])
            fits = worst < 0.5
            choice = jnp.where(fits, float(index), choice)
            flow = jnp.where(fits, need, flow)
    class_ref[...] = jnp.broadcast_to(choice, (8, 128)).astype(jnp.int32)

    left = jnp.where(group == 0, groups - 1, group - 1)
    right = jnp.where(group == groups - 1, 0, group + 1)
    sub1 = lax.broadcasted_iota(jnp.int32, (128, 1), 0)
    lan1 = lax.broadcasted_iota(jnp.int32, (1, 128), 1)

    def at_row(values, index):
        return jnp.sum(jnp.where(sub1 == index, values, 0.0), axis=0, keepdims=True)

    def at_lane(values, index):
        return jnp.sum(jnp.where(lan1 == index, values, 0.0), axis=1, keepdims=True)

    f_here, f_left = at_row(flow, group), at_row(flow, left)
    n1_here, n1_left = at_lane(n1, group), at_lane(n1, left)
    n0_here, n0_right = at_lane(n0, group), at_lane(n0, right)

    cand = cand_ref[...]

    def orbital_of(block, inner):
        b = group + block - 1
        b = jnp.where(b < 0, b + groups, jnp.where(b >= groups, b - groups, b))
        return b * ORB + inner

    row_id = orbital_of(cand[0:1], cand[1:2])
    col_id = orbital_of(cand[2:3], cand[3:4])
    kind = cand[4:5]
    valid = cand[5:6] > 0
    orb = lax.broadcasted_iota(jnp.int32, (norb, 128), 0)
    col_hot = (orb == col_id).astype(F32)
    picked = jnp.dot(m, col_hot, preferred_element_type=F32)
    live = jnp.sum(jnp.where(orb == row_id, picked, 0.0), axis=0, keepdims=True)
    live = jnp.where(valid, live, 0.0)
    rank = jnp.dot(
        jnp.broadcast_to(live, (8, 128)), same_ref[...], preferred_element_type=F32
    )[0:1]
    big = 1e9
    x1 = jnp.minimum(jnp.maximum(f_here, 0.0), n1_here)
    y1 = jnp.minimum(jnp.maximum(f_left, 0.0), n1_left)
    b0 = jnp.maximum(f_here - n1_here, 0.0)
    a0 = jnp.maximum(-f_left, 0.0)
    low_rank = jnp.where(
        kind == 1,
        x1,
        jnp.where(kind == 3, b0, jnp.where(kind == 5, n0_right - jnp.maximum(-f_here, 0.0), 0.0)),
    )
    high_rank = jnp.where(
        kind == 2,
        y1,
        jnp.where(
            kind == 3, n0_here - a0, jnp.where(kind == 4, jnp.maximum(f_left - n1_left, 0.0), big)
        ),
    )
    active = jnp.where((rank >= low_rank) & (rank < high_rank), live, 0.0)
    place = jnp.dot(
        jnp.broadcast_to(active, (8, 128)), before_ref[...], preferred_element_type=F32
    )[0:1]
    slot = lax.broadcasted_iota(jnp.int32, (slots, 128), 0).astype(F32)
    hot = jnp.where(place == slot, active, 0.0)
    first = (cand[0:1] * ORB + cand[1:2]).astype(F32)
    second = (cand[2:3] * ORB + cand[3:4]).astype(F32)
    i_of = jnp.sum(hot * first, axis=1, keepdims=True)
    j_of = jnp.sum(hot * second, axis=1, keepdims=True)
    w_of = jnp.sum(hot, axis=1, keepdims=True)
    lane_s = lax.broadcasted_iota(jnp.int32, (slots, 128), 1)
    tab_ref[...] = jnp.where(lane_s == 0, i_of, jnp.where(lane_s == 1, j_of, 0.0)).astype(jnp.int32)
    w_cross = jnp.where(i_of == j_of, 0.0, w_of)
    for q in range(3 * ORB):
        coef_ref[0, q] = jnp.broadcast_to(jnp.where(i_of == q, w_of, 0.0), (slots, 128))
        coef_ref[1, q] = jnp.broadcast_to(jnp.where(j_of == q, w_cross, 0.0), (slots, 128))


def plan(slots, classes, pair_mask):
    table, same_kind, before = candidates()
    vmem = pl.BlockSpec(memory_space=pltpu.VMEM)
    return pl.pallas_call(
        functools.partial(plan_kernel, slots, classes),
        out_shape=(
            jax.ShapeDtypeStruct((slots, 128), jnp.int32),
            jax.ShapeDtypeStruct((2, 3 * ORB, slots, 128), F32),
            jax.ShapeDtypeStruct((8, 128), jnp.int32),
        ),
        in_specs=[vmem] * 4,
        out_specs=(vmem, vmem, vmem),
        name="plan",
    )(pair_mask, jnp.asarray(table), jnp.asarray(same_kind), jnp.asarray(before))


def split_sum(low_mask, tall):
    outs = []
    for t in range(tall.shape[1] // 128):
        top0, bot0, top1, bot1 = (
            tall[32 * u : 32 * (u + 1), t * 128 : (t + 1) * 128] for u in range(4)
        )
        outs.append(
            jnp.where(low_mask, top0, bot1) + pltpu.roll(jnp.where(low_mask, bot0, top1), 64, 1)
        )
    return outs


def mega_kernel(edge_slots, inner_slots, *refs):
    rounds = (max(edge_slots, inner_slots) + 3) // 4
    (tab, coef, ax_ref, wz_ref, ay_ref, ai_ref, orb_hbm, out_ref) = refs[:8]
    orbs = refs[8 : 8 + NC]
    sums = refs[8 + NC : 8 + 2 * NC]
    back = refs[8 + 2 * NC : 8 + 3 * NC]
    (rho, cube, work, vout, vrecv, ktab) = refs[8 + 3 * NC : 14 + 3 * NC]
    (lsem, z1s, z1r, x1s, x1r, x2s, x2r, z2s, z2r) = refs[14 + 3 * NC :]

    groups = lax.axis_size("band")
    band = lax.axis_index("band")
    me = lax.axis_index("grid")
    on_edge = 1 - lax.rem((lax.rem(band, 4) + 1) // 2, 2)
    halves = inner_slots // 2 + on_edge * (edge_slots // 2 - inner_slots // 2)
    chip, core = me // 2, lax.rem(me, 2)
    mine = (halves - core + 1) // 2
    others = (halves + core) // 2
    left = lax.rem(band + groups - 1, groups)
    right = lax.rem(band + 1, groups)
    peers = {
        0: me,
        1: me + 1 - 2 * lax.rem(me, 2),
        2: lax.rem(me + 2, 4),
        3: 3 - me,
    }

    def local_copy(c):
        return pltpu.make_async_copy(
            orb_hbm.at[:, :, pl.ds(c * CL, CL)], orbs[c].at[pl.ds(ORB, ORB)], lsem.at[c]
        )

    for c in range(NC):
        local_copy(c).start()

    barrier = pltpu.get_barrier_semaphore()
    for target in (left, right):
        pl.semaphore_signal(barrier, inc=1, device_id=(target, me), device_id_type=MESH)
    for k in (1, 2, 3):
        pl.semaphore_signal(barrier, inc=1, device_id=(band, peers[k]), device_id_type=MESH)
    pl.semaphore_wait(barrier, 5)

    def z1(side, c):
        return pltpu.make_async_remote_copy(
            src_ref=orbs[c].at[pl.ds(ORB, ORB)],
            dst_ref=orbs[c].at[pl.ds(2 * ORB if side == 0 else 0, ORB)],
            send_sem=z1s.at[side, c],
            recv_sem=z1r.at[side, c],
            device_id=(left if side == 0 else right, me),
            device_id_type=MESH,
        )

    for c in range(NC):
        local_copy(c).wait()
        z1(0, c).start()
        z1(1, c).start()

    low_mask = lax.broadcasted_iota(jnp.int32, (32, 128), 1) < 64

    def signed(k):
        return jnp.where(k < NG // 2, k, k - NG)

    lane = lax.broadcasted_iota(jnp.int32, (32, 128), 1)
    sub = lax.broadcasted_iota(jnp.int32, (32, 128), 0)
    fy = signed(sub + jnp.where(low_mask, 0, 32))
    fz = signed(jnp.where(low_mask, lane, lane - 64))
    flat = fy * fy + fz * fz

    def fill(kx, carry):
        fx = signed(kx)
        squared = flat + fx * fx
        safe = jnp.maximum(squared, 1).astype(F32)
        ktab[pl.ds(pl.multiple_of(kx * 32, 32), 32), :] = jnp.where(
            squared > 0, (BOX * BOX / np.pi) / safe, 0.0
        )
        return carry

    lax.fori_loop(0, NG, fill, 0)

    def x1(k, r, c):
        return pltpu.make_async_remote_copy(
            src_ref=rho.at[k - 1, r, pl.ds(c * CY, CY)],
            dst_ref=cube.at[r, pl.ds(c * CY, CY), me],
            send_sem=x1s.at[k - 1, r, c],
            recv_sem=x1r.at[k - 1, r, c],
            device_id=(band, peers[k]),
            device_id_type=MESH,
        )

    def x2(k, r, c):
        return pltpu.make_async_remote_copy(
            src_ref=vout.at[r, pl.ds(c * CY, CY), peers[k]],
            dst_ref=vrecv.at[k - 1, r, pl.ds(c * CY, CY)],
            send_sem=x2s.at[k - 1, r, c],
            recv_sem=x2r.at[k - 1, r, c],
            device_id=(band, peers[k]),
            device_id_type=MESH,
        )

    def z2(side, c):
        return pltpu.make_async_remote_copy(
            src_ref=sums[c].at[pl.ds(0 if side == 0 else 2 * ORB, ORB)],
            dst_ref=back[c].at[1 if side == 0 else 0],
            send_sem=z2s.at[side, c],
            recv_sem=z2r.at[side, c],
            device_id=(left if side == 0 else right, me),
            device_id_type=MESH,
        )

    def lanes(y):
        return pl.ds(pl.multiple_of(y * 128, 128), 128)

    def slot_of(k, r):
        half = 2 * r + (core if k in (0, 2) else 1 - core)
        return 2 * half + (chip if k in (0, 1) else 1 - chip)

    def densities(c, r, targets):
        ids = []
        for k in targets:
            slot = slot_of(k, r)
            ids.append((k, tab[slot, 0], tab[slot, 1]))

        def one_tile(y, carry):
            for k, i, j in ids:
                value = orbs[c][i, :, lanes(y)] * orbs[c][j, :, lanes(y)]
                if k == 0:
                    cube[r, c * CY + y, me] = value
                else:
                    rho[k - 1, r, c * CY + y] = value
            return carry

        lax.fori_loop(0, CY, one_tile, 0)
        for k in targets:
            if k:
                x1(k, r, c).start()

    order = [(0, 0), (0, 1), (1, 0), (2, 0), (1, 1), (3, 0), (2, 1), (3, 1)]
    order += [(c, r) for r in range(2, rounds) for c in range(NC)]
    seen = set()
    for c, r in order:
        if r >= rounds:
            continue
        if c not in seen:
            seen.add(c)
            z1(0, c).wait_recv()
            z1(1, c).wait_recv()

        @pl.when(r < mine)
        def _():
            densities(c, r, (2, 0))

        @pl.when(r < others)
        def _():
            densities(c, r, (3, 1))

    ax = ax_ref[...]
    wz = wz_ref[...]

    def along_z(tiles):
        stacked = jnp.concatenate(tiles, axis=0)
        hi, lo = hi_lo(stacked)
        wide = jnp.dot(jnp.concatenate([hi, lo], axis=1), wz, preferred_element_type=F32)
        both = wide[:, :128] + wide[:, 128:]
        return [both[t * NG : (t + 1) * NG] for t in range(len(tiles))]

    def along_x(tiles):
        outs = []
        for t in range(0, len(tiles), 2):
            hi, lo = hi_lo(jnp.concatenate([tiles[t], tiles[t + 1]], axis=1))
            wide = jnp.dot(ax, jnp.concatenate([hi, hi, lo], axis=0), preferred_element_type=F32)
            outs += [wide[:, :128], wide[:, 128:]]
        return outs

    def work_rows(r, y):
        return pl.ds(pl.multiple_of((r * 32 + y) * PITCH, 8), NG)

    def forward(r, c):
        for k in (1, 2, 3):
            x1(k, r, c).wait_recv()
        tiles = [cube[r, c * CY + t].reshape(NG, 128) for t in range(CY)]
        tiles = along_z(along_x(tiles))
        for t in range(CY):
            work[work_rows(r, c * CY + t), :] = tiles[t]

    def spread(tiles):
        hi, lo = hi_lo(jnp.concatenate(tiles, axis=1))
        return jnp.concatenate([hi, hi, lo], axis=0)

    ay = ay_ref[...]
    ai = ai_ref[...]

    def middle(r, g):
        base = r * (32 * PITCH) + g * KX
        for t in range(0, KX, 2):
            tiles = [work[pl.ds(base + t + u, 32, stride=PITCH), :] for u in range(2)]
            tiles = split_sum(low_mask, jnp.dot(ay, spread(tiles), preferred_element_type=F32))
            tiles = [
                tiles[u] * ktab[pl.ds(pl.multiple_of((g * KX + t + u) * 32, 32), 32), :]
                for u in range(2)
            ]
            tiles = split_sum(low_mask, jnp.dot(ai, spread(tiles), preferred_element_type=F32))
            for u in range(2):
                work[pl.ds(base + t + u, 32, stride=PITCH), :] = tiles[u]

    def inverse(r, c):
        tiles = [work[work_rows(r, c * CY + t), :] for t in range(CY)]
        tiles = along_x(along_z(tiles))
        for t in range(CY):
            vout[r, c * CY + t] = tiles[t].reshape(4, 16, 128)
        for k in (2, 3, 1):
            x2(k, r, c).start()

    def looped(count, step):
        def body(i, carry):
            step(i)
            return carry

        lax.fori_loop(0, count, body, 0)

    @functools.partial(looped, mine)
    def _(r):
        looped(NC, functools.partial(forward, r))
        looped(NG // KX, functools.partial(middle, r))
        looped(NC, functools.partial(inverse, r))

    for c in range(NC):
        sums[c][...] = jnp.zeros_like(sums[c])

    def accumulate(c, r, sources):
        ids = []
        for k in sources:
            slot = slot_of(k, r)
            ids.append((k, slot, tab[slot, 0], tab[slot, 1]))
            if k:
                x2(k, r, c).wait_recv()

        @functools.partial(looped, CY)
        def _(y):
            totals = [sums[c][q, :, lanes(y)] for q in range(3 * ORB)]
            for k, slot, i, j in ids:
                if k == 0:
                    v = vout[r, c * CY + y, me]
                else:
                    v = vrecv[k - 1, r, c * CY + y]
                on_i = v * orbs[c][j, :, lanes(y)]
                on_j = v * orbs[c][i, :, lanes(y)]
                for q in range(3 * ORB):
                    totals[q] = totals[q] + (
                        coef[0, q, pl.ds(slot, 1), :] * on_i
                        + coef[1, q, pl.ds(slot, 1), :] * on_j
                    )
            for q in range(3 * ORB):
                sums[c][q, :, lanes(y)] = totals[q]

    def both(c, r):
        @pl.when(r < mine)
        def _():
            accumulate(c, r, (0, 2))

        @pl.when(r < others)
        def _():
            accumulate(c, r, (1, 3))

    last = (halves + 1) // 2 - 1

    @functools.partial(looped, last)
    def _(r):
        for c in range(NC):
            both(c, r)

    for c in range(NC):
        both(c, last)
        z2(0, c).start()
        z2(1, c).start()

    for c in range(NC):
        z2(0, c).wait_recv()
        z2(1, c).wait_recv()
        for a in range(ORB):
            out_ref[a, :, pl.ds(c * CL, CL)] = -MIXING * (
                sums[c][ORB + a] + (back[c][0, a] + back[c][1, a])
            )

    for c in range(NC):
        for side in range(2):
            z1(side, c).wait_send()
            z2(side, c).wait_send()

    @functools.partial(looped, mine)
    def _(r):
        for c in range(NC):
            x1(2, r, c).wait_send()
            for k in (1, 2, 3):
                x2(k, r, c).wait_send()

    @functools.partial(looped, others)
    def _(r):
        for c in range(NC):
            for k in (1, 3):
                x1(k, r, c).wait_send()


def mega(slots, collective_id, tab, coef, orbitals):
    rounds = (max(slots) + 3) // 4
    ax, wz, ay, ai = tables()
    vmem = pl.BlockSpec(memory_space=pltpu.VMEM)
    planes = orbitals.shape[1]
    dma = pltpu.SemaphoreType.DMA
    return pl.pallas_call(
        functools.partial(mega_kernel, *slots),
        out_shape=jax.ShapeDtypeStruct(orbitals.shape, F32),
        in_specs=[pl.BlockSpec(memory_space=pltpu.SMEM)]
        + [vmem] * 5
        + [pl.BlockSpec(memory_space=pl.ANY)],
        out_specs=vmem,
        scratch_shapes=[pltpu.VMEM((3 * ORB, planes, CL), F32) for _ in range(2 * NC)]
        + [pltpu.VMEM((2, ORB, planes, CL), F32) for _ in range(NC)]
        + [
            pltpu.VMEM((3, rounds, 32, planes, 128), F32),
            pltpu.VMEM((rounds, 32, 4, planes, 128), F32),
            pltpu.VMEM((rounds * 32 * PITCH, 128), F32),
            pltpu.VMEM((rounds, 32, 4, planes, 128), F32),
            pltpu.VMEM((3, rounds, 32, planes, 128), F32),
            pltpu.VMEM((NG * 32, 128), F32),
            dma((NC,)),
            dma((2, NC)),
            dma((2, NC)),
            dma((3, rounds, NC)),
            dma((3, rounds, NC)),
            dma((3, rounds, NC)),
            dma((3, rounds, NC)),
            dma((2, NC)),
            dma((2, NC)),
        ],
        compiler_params=pltpu.CompilerParams(
            collective_id=collective_id, has_side_effects=True, vmem_limit_bytes=56 * 1024 * 1024
        ),
        name="mega%d_%d" % slots,
    )(
        tab,
        coef,
        jnp.asarray(ax),
        jnp.asarray(wz),
        jnp.asarray(ay),
        jnp.asarray(ai),
        orbitals,
    )


def local(orbitals, pair_mask):
    tab, coef, index = plan(16, CLASSES, pair_mask)
    branches = [functools.partial(mega, slots, 3 + n) for n, slots in enumerate(CLASSES)]
    if len(branches) == 1:
        return branches[0](tab, coef, orbitals)
    return lax.switch(index[0, 0], branches, tab, coef, orbitals)


def solution(mesh):
    return jax.shard_map(
        local,
        mesh=mesh,
        in_specs=(P("band", "grid", None), P()),
        out_specs=P("band", "grid", None),
        check_vma=False,
    )
```

```python
import functools

import jax
import jax.numpy as jnp
import numpy as np
from jax import lax
from jax.experimental import pallas as pl
from jax.experimental.pallas import tpu as pltpu
from jax.sharding import PartitionSpec as P

NG = 64
ORB = 3
MIXING = 0.25
BOX = 16.0
NC = 4
CY = 32 // NC
CL = CY * 128
EARLY = 3 * NC // 4
KX = 16
CLASSES = ((6, 10), (8, 12), (9, 12), (12, 12))
PITCH = 72
MESH = pl.DeviceIdType.MESH
F32 = jnp.float32
BF16 = jnp.bfloat16


def hi_lo(values):
    hi = values.astype(BF16)
    return hi, (values - hi.astype(F32)).astype(BF16)


def host_hi_lo(values):
    hi = values.astype(np.float32).astype(BF16)
    return hi, (values - hi.astype(np.float64)).astype(np.float32).astype(BF16)


def tables():
    n = np.arange(NG)
    angle = 2.0 * np.pi * ((n[:, None] * n[None, :]) % NG) / NG
    h = (np.cos(angle) + np.sin(angle)) / 8.0
    hh, hl = host_hi_lo(h)
    ax = np.concatenate([hh, hl, hh], axis=1)
    bh, bl = host_hi_lo(np.kron(np.eye(2), h))
    wz = np.block([[bh, bl], [bh, np.zeros_like(bl)]])
    fh, fl = host_hi_lo(np.concatenate([h[:, 0::2], h[:, 1::2]], axis=0))
    ay = np.concatenate([fh, fl, fh], axis=1)
    back = np.concatenate([h[0::2], h[1::2]], axis=0)
    gh, gl = host_hi_lo(np.concatenate([back[:, :32], back[:, 32:]], axis=0))
    ai = np.concatenate([gh, gl, gh], axis=1)
    return ax, wz, ay, ai


def candidates():
    rows = []
    for first, second, same, kind in (
        (0, 2, False, 0),
        (1, 2, False, 1),
        (0, 1, False, 2),
        (1, 1, True, 3),
        (0, 0, True, 4),
        (2, 2, True, 5),
    ):
        for a in range(ORB):
            for b in range(ORB):
                if not same or a <= b:
                    rows.append((first, a, second, b, kind, 1))
    table = np.zeros((8, 128), np.int32)
    for c, row in enumerate(rows):
        table[:6, c] = row
    kind = np.where(table[5] > 0, table[4], -1)
    before = np.arange(128)[:, None] < np.arange(128)[None, :]
    same_kind = before & (kind[:, None] == kind[None, :])
    return table, same_kind.astype(np.float32), before.astype(np.float32)


def plan_kernel(slots, classes, mask_ref, cand_ref, same_ref, before_ref, tab_ref, coef_ref, class_ref):
    norb = mask_ref.shape[0]
    groups = norb // ORB
    group = lax.axis_index("band")
    m = mask_ref[...].astype(F32)
    rows = lax.broadcasted_iota(jnp.int32, (norb, norb), 0)
    cols = lax.broadcasted_iota(jnp.int32, (norb, norb), 1)
    brow = (rows * 21846) >> 16
    bcol = (cols * 21846) >> 16
    sep = jnp.where(bcol >= brow, bcol - brow, bcol - brow + groups)

    def row_sum(keep):
        return jnp.sum(jnp.where(keep, m, 0.0), axis=1, keepdims=True)

    r0 = row_sum((sep == 0) & (rows <= cols))
    r1 = row_sum(sep == 1)
    r2 = row_sum(sep == 2)
    gb = (lax.broadcasted_iota(jnp.int32, (norb, 128), 0) * 21846) >> 16
    lane = lax.broadcasted_iota(jnp.int32, (norb, 128), 1)
    nxt = jnp.where(gb == groups - 1, 0, gb + 1)
    prv = jnp.where(gb == 0, groups - 1, gb - 1)

    def to_lanes(values, place):
        return jnp.sum(jnp.where(place == lane, values, 0.0), axis=0, keepdims=True)

    n0 = to_lanes(r0, gb)
    n0_next = to_lanes(r0, prv)
    n1 = to_lanes(r1, gb)
    n2_prev = to_lanes(r2, nxt)
    load = n2_prev + n1 + n0
    sub = lax.broadcasted_iota(jnp.int32, (128, 128), 0)
    lan = lax.broadcasted_iota(jnp.int32, (128, 128), 1)
    sub1 = lax.broadcasted_iota(jnp.int32, (128, 1), 0)
    lan1 = lax.broadcasted_iota(jnp.int32, (1, 128), 1)
    eye = sub == lan

    def to_rows(values):
        return jnp.sum(jnp.where(eye, values, 0.0), axis=1, keepdims=True)

    low = -n0_next
    high = to_rows(n1 + n0)
    prev_rows = to_rows(n2_prev)
    load_rows = jnp.where(sub < groups, to_rows(load), 0.0)
    prefix = jnp.sum(jnp.where(sub <= lan, load_rows, 0.0), axis=0, keepdims=True)
    total = jnp.sum(load_rows, axis=0, keepdims=True)
    path = to_rows(prefix) - prefix + jnp.where(sub < lan, total, 0.0) + low
    path = jnp.where(lan < groups, path, -1e9)

    def edges_to(m):
        return 2 * (m // 4) + 1 + lax.rem(m, 4) // 3

    def held_to(m, edge, inner):
        return (inner * (m + 1) + (edge - inner) * edges_to(m)).astype(F32)

    is_edge = lax.rem((lax.rem(sub1, 4) + 1) // 2, 2) == 0
    choice, flow = None, None
    for index in reversed(range(len(classes))):
        edge, inner = classes[index]
        held = float((edge + inner) * (groups // 2))
        need = path - held_to(sub1, edge, inner) + held_to(lan1, edge, inner)
        need = jnp.max(jnp.where(sub < lan, need - held, need), axis=1, keepdims=True)
        if choice is None:
            choice, flow = jnp.full((1, 1), float(index), F32), need
        else:
            over = jnp.maximum(need - high, prev_rows - jnp.where(is_edge, float(edge), float(inner)))
            over = jnp.where(sub1 < groups, over, -1e9)
            worst = jnp.maximum(jnp.max(over, axis=0, keepdims=True), total[:, :1] - held)
            fits = worst < 0.5
            choice = jnp.where(fits, float(index), choice)
            flow = jnp.where(fits, need, flow)
    class_ref[0] = jnp.max(choice).astype(jnp.int32)

    left = jnp.where(group == 0, groups - 1, group - 1)
    right = jnp.where(group == groups - 1, 0, group + 1)

    def at_row(values, index):
        return jnp.sum(jnp.where(sub1 == index, values, 0.0), axis=0, keepdims=True)

    def at_lane(values, index):
        return jnp.sum(jnp.where(lan1 == index, values, 0.0), axis=1, keepdims=True)

    f_here, f_left = at_row(flow, group), at_row(flow, left)
    n1_here, n1_left = at_lane(n1, group), at_lane(n1, left)
    n0_here, n0_right = at_lane(n0, group), at_lane(n0, right)

    cand = cand_ref[...]

    def orbital_of(block, inner):
        b = group + block - 1
        b = jnp.where(b < 0, b + groups, jnp.where(b >= groups, b - groups, b))
        return b * ORB + inner

    row_id = orbital_of(cand[0:1], cand[1:2])
    col_id = orbital_of(cand[2:3], cand[3:4])
    kind = cand[4:5]
    valid = cand[5:6] > 0
    orb = lax.broadcasted_iota(jnp.int32, (norb, 128), 0)
    col_hot = (orb == col_id).astype(F32)
    picked = jnp.dot(m, col_hot, preferred_element_type=F32)
    live = jnp.sum(jnp.where(orb == row_id, picked, 0.0), axis=0, keepdims=True)
    live = jnp.where(valid, live, 0.0)
    rank = jnp.dot(
        jnp.broadcast_to(live, (8, 128)), same_ref[...], preferred_element_type=F32
    )[0:1]
    big = 1e9
    x1 = jnp.minimum(jnp.maximum(f_here, 0.0), n1_here)
    y1 = jnp.minimum(jnp.maximum(f_left, 0.0), n1_left)
    b0 = jnp.maximum(f_here - n1_here, 0.0)
    a0 = jnp.maximum(-f_left, 0.0)
    low_rank = jnp.where(
        kind == 1,
        x1,
        jnp.where(kind == 3, b0, jnp.where(kind == 5, n0_right - jnp.maximum(-f_here, 0.0), 0.0)),
    )
    high_rank = jnp.where(
        kind == 2,
        y1,
        jnp.where(
            kind == 3, n0_here - a0, jnp.where(kind == 4, jnp.maximum(f_left - n1_left, 0.0), big)
        ),
    )
    active = jnp.where((rank >= low_rank) & (rank < high_rank), live, 0.0)
    place = jnp.dot(
        jnp.broadcast_to(active, (8, 128)), before_ref[...], preferred_element_type=F32
    )[0:1]
    slot = lax.broadcasted_iota(jnp.int32, (slots, 128), 0).astype(F32)
    hot = jnp.where(place == slot, active, 0.0)
    first = (cand[0:1] * ORB + cand[1:2]).astype(F32)
    second = (cand[2:3] * ORB + cand[3:4]).astype(F32)
    i_of = jnp.sum(hot * first, axis=1, keepdims=True)
    j_of = jnp.sum(hot * second, axis=1, keepdims=True)
    w_of = jnp.sum(hot, axis=1, keepdims=True)
    lane_s = lax.broadcasted_iota(jnp.int32, (slots, 128), 1)
    tab_ref[...] = jnp.where(lane_s == 0, i_of, jnp.where(lane_s == 1, j_of, 0.0)).astype(jnp.int32)
    w_cross = jnp.where(i_of == j_of, 0.0, w_of)
    for q in range(3 * ORB):
        coef_ref[0, q] = jnp.broadcast_to(jnp.where(i_of == q, w_of, 0.0), (slots, 128))
        coef_ref[1, q] = jnp.broadcast_to(jnp.where(j_of == q, w_cross, 0.0), (slots, 128))


def plan(slots, classes, pair_mask):
    table, same_kind, before = candidates()
    vmem = pl.BlockSpec(memory_space=pltpu.VMEM)
    return pl.pallas_call(
        functools.partial(plan_kernel, slots, classes),
        out_shape=(
            jax.ShapeDtypeStruct((slots, 128), jnp.int32),
            jax.ShapeDtypeStruct((2, 3 * ORB, slots, 128), F32),
            jax.ShapeDtypeStruct((1,), jnp.int32),
        ),
        in_specs=[vmem] * 4,
        out_specs=(vmem, vmem, pl.BlockSpec(memory_space=pltpu.SMEM)),
        name="plan",
    )(pair_mask, jnp.asarray(table), jnp.asarray(same_kind), jnp.asarray(before))


def split_sum(low_mask, tall):
    outs = []
    for t in range(tall.shape[1] // 128):
        top0, bot0, top1, bot1 = (
            tall[32 * u : 32 * (u + 1), t * 128 : (t + 1) * 128] for u in range(4)
        )
        outs.append(
            jnp.where(low_mask, top0, bot1) + pltpu.roll(jnp.where(low_mask, bot0, top1), 64, 1)
        )
    return outs


def mega_kernel(edge_slots, inner_slots, *refs):
    rounds = (max(edge_slots, inner_slots) + 3) // 4
    (tab, coef, ax_ref, wz_ref, ay_ref, ai_ref, orb_hbm, out_ref) = refs[:8]
    orbs = refs[8 : 8 + NC]
    sums = refs[8 + NC : 8 + 2 * NC]
    back = refs[8 + 2 * NC : 8 + 3 * NC]
    (rho, cube, work, vout, vrecv, ktab) = refs[8 + 3 * NC : 14 + 3 * NC]
    (lsem, z1s, z1r, x1s, x1r, x2s, x2r, z2s, z2r) = refs[14 + 3 * NC :]

    groups = lax.axis_size("band")
    band = lax.axis_index("band")
    me = lax.axis_index("grid")
    z = lax.rem(band, 4)
    on_edge = 1 - lax.rem((z + 1) // 2, 2)
    held = inner_slots + on_edge * (edge_slots - inner_slots)
    chip, core = me // 2, lax.rem(me, 2)

    def slot_of(k, r):
        return (
            4 * r
            + 2 * (core if k in (0, 2) else 1 - core)
            + (chip if k in (0, 1) else 1 - chip)
        )

    def rounds_of(k):
        return (held + 3 - slot_of(k, 0)) // 4

    left = lax.rem(band + groups - 1, groups)
    right = lax.rem(band + 1, groups)
    peers = {
        0: me,
        1: me + 1 - 2 * lax.rem(me, 2),
        2: lax.rem(me + 2, 4),
        3: 3 - me,
    }

    def local_copy(c):
        return pltpu.make_async_copy(
            orb_hbm.at[:, :, pl.ds(c * CL, CL)], orbs[c].at[pl.ds(ORB, ORB)], lsem.at[c]
        )

    for c in range(NC):
        local_copy(c).start()

    barrier = pltpu.get_barrier_semaphore()
    for target in (left, right):
        pl.semaphore_signal(barrier, inc=1, device_id=(target, me), device_id_type=MESH)
    for k in (1, 2, 3):
        pl.semaphore_signal(barrier, inc=1, device_id=(band, peers[k]), device_id_type=MESH)
    pl.semaphore_wait(barrier, 5)

    def z1(side, c):
        return pltpu.make_async_remote_copy(
            src_ref=orbs[c].at[pl.ds(ORB, ORB)],
            dst_ref=orbs[c].at[pl.ds(2 * ORB if side == 0 else 0, ORB)],
            send_sem=z1s.at[side, c],
            recv_sem=z1r.at[side, c],
            device_id=(left if side == 0 else right, me),
            device_id_type=MESH,
        )

    for c in range(NC):
        local_copy(c).wait()
        z1(0, c).start()
        z1(1, c).start()

    low_mask = lax.broadcasted_iota(jnp.int32, (32, 128), 1) < 64

    def signed(k):
        return jnp.where(k < NG // 2, k, k - NG)

    lane = lax.broadcasted_iota(jnp.int32, (32, 128), 1)
    sub = lax.broadcasted_iota(jnp.int32, (32, 128), 0)
    fy = signed(sub + jnp.where(low_mask, 0, 32))
    fz = signed(jnp.where(low_mask, lane, lane - 64))
    flat = fy * fy + fz * fz

    def fill(kx, carry):
        fx = signed(kx)
        squared = flat + fx * fx
        safe = jnp.maximum(squared, 1).astype(F32)
        ktab[pl.ds(pl.multiple_of(kx * 32, 32), 32), :] = jnp.where(
            squared > 0, (BOX * BOX / np.pi) / safe, 0.0
        )
        return carry

    lax.fori_loop(0, NG, fill, 0)

    def x1(k, r, c):
        return pltpu.make_async_remote_copy(
            src_ref=rho.at[k - 1, r, pl.ds(c * CY, CY)],
            dst_ref=cube.at[r, pl.ds(c * CY, CY), me],
            send_sem=x1s.at[k - 1, r, c],
            recv_sem=x1r.at[k - 1, r, c],
            device_id=(band, peers[k]),
            device_id_type=MESH,
        )

    def x2(k, r, c):
        return pltpu.make_async_remote_copy(
            src_ref=vout.at[r, pl.ds(c * CY, CY), peers[k]],
            dst_ref=vrecv.at[k - 1, r, pl.ds(c * CY, CY)],
            send_sem=x2s.at[k - 1, r, c],
            recv_sem=x2r.at[k - 1, r, c],
            device_id=(band, peers[k]),
            device_id_type=MESH,
        )

    def z2(side, c):
        return pltpu.make_async_remote_copy(
            src_ref=sums[c].at[pl.ds(0 if side == 0 else 2 * ORB, ORB)],
            dst_ref=back[c].at[1 if side == 0 else 0],
            send_sem=z2s.at[side, c],
            recv_sem=z2r.at[side, c],
            device_id=(left if side == 0 else right, me),
            device_id_type=MESH,
        )

    def lanes(y):
        return pl.ds(pl.multiple_of(y * 128, 128), 128)

    def densities(c, r, k):
        slot = slot_of(k, r)
        i, j = tab[slot, 0], tab[slot, 1]

        def one_tile(y, carry):
            value = orbs[c][i, :, lanes(y)] * orbs[c][j, :, lanes(y)]
            if k == 0:
                cube[r, c * CY + y, me] = value
            else:
                rho[k - 1, r, c * CY + y] = value
            return carry

        lax.fori_loop(0, CY, one_tile, 0, unroll=4)
        if k:
            x1(k, r, c).start()

    order = []
    for c in range(NC):
        order.append((c, 0))
        if c % 2 == 0:
            order.append((c // 2, 1))
    order += [(c, 1) for c in range((NC + 1) // 2, NC)]
    order += [(c, r) for r in range(2, rounds) for c in range(NC)]
    seen = set()
    for c, r in order:
        if r >= rounds:
            continue
        if c not in seen:
            seen.add(c)
            z1(0, c).wait_recv()
            z1(1, c).wait_recv()

        for k in (2, 3, 1, 0):

            @pl.when(slot_of(k, r) < held)
            def _():
                densities(c, r, k)

    ax = ax_ref[...]
    wz = wz_ref[...]

    def along_z(tiles):
        stacked = jnp.concatenate(tiles, axis=0)
        hi, lo = hi_lo(stacked)
        wide = jnp.dot(jnp.concatenate([hi, lo], axis=1), wz, preferred_element_type=F32)
        both = wide[:, :128] + wide[:, 128:]
        return [both[t * NG : (t + 1) * NG] for t in range(len(tiles))]

    def along_x(tiles):
        outs = []
        for t in range(0, len(tiles), 2):
            hi, lo = hi_lo(jnp.concatenate([tiles[t], tiles[t + 1]], axis=1))
            wide = jnp.dot(ax, jnp.concatenate([hi, hi, lo], axis=0), preferred_element_type=F32)
            outs += [wide[:, :128], wide[:, 128:]]
        return outs

    def work_rows(r, y):
        return pl.ds(pl.multiple_of((r * 32 + y) * PITCH, 8), NG)

    def forward(r, c):
        for k in (1, 2, 3):
            x1(k, r, c).wait_recv()
        tiles = [cube[r, c * CY + t].reshape(NG, 128) for t in range(CY)]
        tiles = along_z(along_x(tiles))
        for t in range(CY):
            work[work_rows(r, c * CY + t), :] = tiles[t]

    def spread(tiles):
        hi, lo = hi_lo(jnp.concatenate(tiles, axis=1))
        return jnp.concatenate([hi, hi, lo], axis=0)

    ay = ay_ref[...]
    ai = ai_ref[...]

    def middle(r, g):
        base = r * (32 * PITCH) + g * KX
        for t in range(0, KX, 2):
            tiles = [work[pl.ds(base + t + u, 32, stride=PITCH), :] for u in range(2)]
            tiles = split_sum(low_mask, jnp.dot(ay, spread(tiles), preferred_element_type=F32))
            tiles = [
                tiles[u] * ktab[pl.ds(pl.multiple_of((g * KX + t + u) * 32, 32), 32), :]
                for u in range(2)
            ]
            tiles = split_sum(low_mask, jnp.dot(ai, spread(tiles), preferred_element_type=F32))
            for u in range(2):
                work[pl.ds(base + t + u, 32, stride=PITCH), :] = tiles[u]

    def inverse(r, c):
        tiles = [work[work_rows(r, c * CY + t), :] for t in range(CY)]
        tiles = along_x(along_z(tiles))
        for t in range(CY):
            vout[r, c * CY + t] = tiles[t].reshape(4, 16, 128)

    def return_chunk(r, c):
        for k in (2, 3, 1):
            x2(k, r, c).start()

    def looped(count, step):
        def body(i, carry):
            step(i)
            return carry

        lax.fori_loop(0, count, body, 0)

    @functools.partial(looped, rounds_of(0))
    def _(r):
        looped(NC, functools.partial(forward, r))
        looped(NG // KX, functools.partial(middle, r))

        @functools.partial(looped, NC)
        def _(c):
            inverse(r, c)

            @pl.when((c < EARLY) | (r == rounds_of(0) - 1))
            def _():
                return_chunk(r, c)

            @pl.when((c >= EARLY) & (r == rounds_of(0) - 1))
            def _():
                looped(r, lambda before: return_chunk(before, c))

    for c in range(NC):
        sums[c][...] = jnp.zeros_like(sums[c])

    def accumulate(c, r, k):
        slot = slot_of(k, r)
        i, j = tab[slot, 0], tab[slot, 1]
        if k:
            x2(k, r, c).wait_recv()

        @functools.partial(looped, CY)
        def _(y):
            if k == 0:
                v = vout[r, c * CY + y, me]
            else:
                v = vrecv[k - 1, r, c * CY + y]
            on_i = v * orbs[c][j, :, lanes(y)]
            on_j = v * orbs[c][i, :, lanes(y)]
            for q in range(3 * ORB):
                sums[c][q, :, lanes(y)] += (
                    coef[0, q, pl.ds(slot, 1), :] * on_i + coef[1, q, pl.ds(slot, 1), :] * on_j
                )

    def both(c, r):
        for k in (0, 1, 2, 3):

            @pl.when(slot_of(k, r) < held)
            def _():
                accumulate(c, r, k)

    last = (held + 3) // 4 - 1

    @functools.partial(looped, last)
    def _(r):
        for c in range(EARLY):
            both(c, r)

    for c in range(NC):
        if c >= EARLY:
            looped(last, functools.partial(both, c))
        both(c, last)
        z2(0, c).start()
        z2(1, c).start()

    for c in range(NC):
        z2(0, c).wait_recv()
        z2(1, c).wait_recv()
        for a in range(ORB):
            out_ref[a, :, pl.ds(c * CL, CL)] = -MIXING * (
                sums[c][ORB + a] + (back[c][0, a] + back[c][1, a])
            )

    for c in range(NC):
        for side in range(2):
            z1(side, c).wait_send()
            z2(side, c).wait_send()

    for k in (1, 2, 3):

        @functools.partial(looped, rounds_of(k))
        def _(r):
            for c in range(NC):
                x1(k, r, c).wait_send()

    @functools.partial(looped, rounds_of(0))
    def _(r):
        for c in range(NC):
            for k in (1, 2, 3):
                x2(k, r, c).wait_send()


def mega(slots, collective_id, tab, coef, orbitals):
    rounds = (max(slots) + 3) // 4
    ax, wz, ay, ai = tables()
    vmem = pl.BlockSpec(memory_space=pltpu.VMEM)
    planes = orbitals.shape[1]
    dma = pltpu.SemaphoreType.DMA
    return pl.pallas_call(
        functools.partial(mega_kernel, *slots),
        out_shape=jax.ShapeDtypeStruct(orbitals.shape, F32),
        in_specs=[pl.BlockSpec(memory_space=pltpu.SMEM)]
        + [vmem] * 5
        + [pl.BlockSpec(memory_space=pl.ANY)],
        out_specs=vmem,
        scratch_shapes=[pltpu.VMEM((3 * ORB, planes, CL), F32) for _ in range(2 * NC)]
        + [pltpu.VMEM((2, ORB, planes, CL), F32) for _ in range(NC)]
        + [
            pltpu.VMEM((3, rounds, 32, planes, 128), F32),
            pltpu.VMEM((rounds, 32, 4, planes, 128), F32),
            pltpu.VMEM((rounds * 32 * PITCH, 128), F32),
            pltpu.VMEM((rounds, 32, 4, planes, 128), F32),
            pltpu.VMEM((3, rounds, 32, planes, 128), F32),
            pltpu.VMEM((NG * 32, 128), F32),
            dma((NC,)),
            dma((2, NC)),
            dma((2, NC)),
            dma((3, rounds, NC)),
            dma((3, rounds, NC)),
            dma((3, rounds, NC)),
            dma((3, rounds, NC)),
            dma((2, NC)),
            dma((2, NC)),
        ],
        compiler_params=pltpu.CompilerParams(
            collective_id=collective_id, has_side_effects=True, vmem_limit_bytes=56 * 1024 * 1024
        ),
        name="mega%d_%d" % slots,
    )(
        tab,
        coef,
        jnp.asarray(ax),
        jnp.asarray(wz),
        jnp.asarray(ay),
        jnp.asarray(ai),
        orbitals,
    )


def local(orbitals, pair_mask):
    tab, coef, index = plan(16, CLASSES, pair_mask)
    branches = [functools.partial(mega, slots, 3 + n) for n, slots in enumerate(CLASSES)]
    if len(branches) == 1:
        return branches[0](tab, coef, orbitals)
    return lax.switch(index[0], branches, tab, coef, orbitals)


def solution(mesh):
    return jax.shard_map(
        local,
        mesh=mesh,
        in_specs=(P("band", "grid", None), P()),
        out_specs=P("band", "grid", None),
        check_vma=False,
    )
```

```python
import functools

import jax
import jax.numpy as jnp
import numpy as np
from jax import lax
from jax.experimental import pallas as pl
from jax.experimental.pallas import tpu as pltpu
from jax.sharding import PartitionSpec as P

NG = 64
ORB = 3
MIXING = 0.25
BOX = 16.0
NC = 4
CY = 32 // NC
CL = CY * 128
EARLY = NC // 2
KX = 16
CLASSES = ((6, 10), (6, 11), (8, 12), (9, 12), (12, 12))
PITCH = 72
MESH = pl.DeviceIdType.MESH
F32 = jnp.float32
BF16 = jnp.bfloat16


def hi_lo(values):
    hi = values.astype(BF16)
    return hi, (values - hi.astype(F32)).astype(BF16)


def host_hi_lo(values):
    hi = values.astype(np.float32).astype(BF16)
    return hi, (values - hi.astype(np.float64)).astype(np.float32).astype(BF16)


def tables():
    n = np.arange(NG)
    angle = 2.0 * np.pi * ((n[:, None] * n[None, :]) % NG) / NG
    h = (np.cos(angle) + np.sin(angle)) / 8.0
    hh, hl = host_hi_lo(h)
    ax = np.concatenate([hh, hl, hh], axis=1)
    bh, bl = host_hi_lo(np.kron(np.eye(2), h))
    wz = np.block([[bh, bl], [bh, np.zeros_like(bl)]])
    fh, fl = host_hi_lo(np.concatenate([h[:, 0::2], h[:, 1::2]], axis=0))
    ay = np.concatenate([fh, fl, fh], axis=1)
    back = np.concatenate([h[0::2], h[1::2]], axis=0)
    gh, gl = host_hi_lo(np.concatenate([back[:, :32], back[:, 32:]], axis=0))
    ai = np.concatenate([gh, gl, gh], axis=1)
    return ax, wz, ay, ai


def candidates():
    rows = []
    for first, second, same, kind in (
        (0, 2, False, 0),
        (1, 2, False, 1),
        (0, 1, False, 2),
        (1, 1, True, 3),
        (0, 0, True, 4),
        (2, 2, True, 5),
    ):
        for a in range(ORB):
            for b in range(ORB):
                if not same or a <= b:
                    rows.append((first, a, second, b, kind, 1))
    table = np.zeros((8, 128), np.int32)
    for c, row in enumerate(rows):
        table[:6, c] = row
    kind = np.where(table[5] > 0, table[4], -1)
    before = np.arange(128)[:, None] < np.arange(128)[None, :]
    same_kind = before & (kind[:, None] == kind[None, :])
    return table, same_kind.astype(np.float32), before.astype(np.float32)


def plan_kernel(slots, classes, mask_ref, cand_ref, same_ref, before_ref, tab_ref, coef_ref, class_ref):
    norb = mask_ref.shape[0]
    groups = norb // ORB
    group = lax.axis_index("band")
    m = mask_ref[...].astype(F32)
    rows = lax.broadcasted_iota(jnp.int32, (norb, norb), 0)
    cols = lax.broadcasted_iota(jnp.int32, (norb, norb), 1)
    brow = (rows * 21846) >> 16
    bcol = (cols * 21846) >> 16
    sep = jnp.where(bcol >= brow, bcol - brow, bcol - brow + groups)

    def row_sum(keep):
        return jnp.sum(jnp.where(keep, m, 0.0), axis=1, keepdims=True)

    r0 = row_sum((sep == 0) & (rows <= cols))
    r1 = row_sum(sep == 1)
    r2 = row_sum(sep == 2)
    gb = (lax.broadcasted_iota(jnp.int32, (norb, 128), 0) * 21846) >> 16
    lane = lax.broadcasted_iota(jnp.int32, (norb, 128), 1)
    nxt = jnp.where(gb == groups - 1, 0, gb + 1)
    prv = jnp.where(gb == 0, groups - 1, gb - 1)

    def to_lanes(values, place):
        return jnp.sum(jnp.where(place == lane, values, 0.0), axis=0, keepdims=True)

    n0 = to_lanes(r0, gb)
    n0_next = to_lanes(r0, prv)
    n1 = to_lanes(r1, gb)
    n2_prev = to_lanes(r2, nxt)
    load = n2_prev + n1 + n0
    sub = lax.broadcasted_iota(jnp.int32, (128, 128), 0)
    lan = lax.broadcasted_iota(jnp.int32, (128, 128), 1)
    sub1 = lax.broadcasted_iota(jnp.int32, (128, 1), 0)
    lan1 = lax.broadcasted_iota(jnp.int32, (1, 128), 1)
    eye = sub == lan

    def to_rows(values):
        return jnp.sum(jnp.where(eye, values, 0.0), axis=1, keepdims=True)

    low = -n0_next
    high = to_rows(n1 + n0)
    prev_rows = to_rows(n2_prev)
    load_rows = jnp.where(sub < groups, to_rows(load), 0.0)
    prefix = jnp.sum(jnp.where(sub <= lan, load_rows, 0.0), axis=0, keepdims=True)
    total = jnp.sum(load_rows, axis=0, keepdims=True)
    path = to_rows(prefix) - prefix + jnp.where(sub < lan, total, 0.0) + low
    path = jnp.where(lan < groups, path, -1e9)

    def edges_to(m):
        return 2 * (m // 4) + 1 + lax.rem(m, 4) // 3

    def held_to(m, edge, inner):
        return (inner * (m + 1) + (edge - inner) * edges_to(m)).astype(F32)

    is_edge = lax.rem((lax.rem(sub1, 4) + 1) // 2, 2) == 0
    choice, flow = None, None
    for index in reversed(range(len(classes))):
        edge, inner = classes[index]
        held = float((edge + inner) * (groups // 2))
        need = path - held_to(sub1, edge, inner) + held_to(lan1, edge, inner)
        need = jnp.max(jnp.where(sub < lan, need - held, need), axis=1, keepdims=True)
        if choice is None:
            choice, flow = jnp.full((1, 1), float(index), F32), need
        else:
            over = jnp.maximum(need - high, prev_rows - jnp.where(is_edge, float(edge), float(inner)))
            over = jnp.where(sub1 < groups, over, -1e9)
            worst = jnp.maximum(jnp.max(over, axis=0, keepdims=True), total[:, :1] - held)
            fits = worst < 0.5
            choice = jnp.where(fits, float(index), choice)
            flow = jnp.where(fits, need, flow)
    class_ref[0] = jnp.max(choice).astype(jnp.int32)

    left = jnp.where(group == 0, groups - 1, group - 1)
    right = jnp.where(group == groups - 1, 0, group + 1)

    def at_row(values, index):
        return jnp.sum(jnp.where(sub1 == index, values, 0.0), axis=0, keepdims=True)

    def at_lane(values, index):
        return jnp.sum(jnp.where(lan1 == index, values, 0.0), axis=1, keepdims=True)

    f_here, f_left = at_row(flow, group), at_row(flow, left)
    n1_here, n1_left = at_lane(n1, group), at_lane(n1, left)
    n0_here, n0_right = at_lane(n0, group), at_lane(n0, right)

    cand = cand_ref[...]

    def orbital_of(block, inner):
        b = group + block - 1
        b = jnp.where(b < 0, b + groups, jnp.where(b >= groups, b - groups, b))
        return b * ORB + inner

    row_id = orbital_of(cand[0:1], cand[1:2])
    col_id = orbital_of(cand[2:3], cand[3:4])
    kind = cand[4:5]
    valid = cand[5:6] > 0
    orb = lax.broadcasted_iota(jnp.int32, (norb, 128), 0)
    col_hot = (orb == col_id).astype(F32)
    picked = jnp.dot(m, col_hot, preferred_element_type=F32)
    live = jnp.sum(jnp.where(orb == row_id, picked, 0.0), axis=0, keepdims=True)
    live = jnp.where(valid, live, 0.0)
    rank = jnp.dot(
        jnp.broadcast_to(live, (8, 128)), same_ref[...], preferred_element_type=F32
    )[0:1]
    big = 1e9
    x1 = jnp.minimum(jnp.maximum(f_here, 0.0), n1_here)
    y1 = jnp.minimum(jnp.maximum(f_left, 0.0), n1_left)
    b0 = jnp.maximum(f_here - n1_here, 0.0)
    a0 = jnp.maximum(-f_left, 0.0)
    low_rank = jnp.where(
        kind == 1,
        x1,
        jnp.where(kind == 3, b0, jnp.where(kind == 5, n0_right - jnp.maximum(-f_here, 0.0), 0.0)),
    )
    high_rank = jnp.where(
        kind == 2,
        y1,
        jnp.where(
            kind == 3, n0_here - a0, jnp.where(kind == 4, jnp.maximum(f_left - n1_left, 0.0), big)
        ),
    )
    active = jnp.where((rank >= low_rank) & (rank < high_rank), live, 0.0)
    place = jnp.dot(
        jnp.broadcast_to(active, (8, 128)), before_ref[...], preferred_element_type=F32
    )[0:1]
    slot = lax.broadcasted_iota(jnp.int32, (slots, 128), 0).astype(F32)
    hot = jnp.where(place == slot, active, 0.0)
    first = (cand[0:1] * ORB + cand[1:2]).astype(F32)
    second = (cand[2:3] * ORB + cand[3:4]).astype(F32)
    i_of = jnp.sum(hot * first, axis=1, keepdims=True)
    j_of = jnp.sum(hot * second, axis=1, keepdims=True)
    w_of = jnp.sum(hot, axis=1, keepdims=True)
    lane_s = lax.broadcasted_iota(jnp.int32, (slots, 128), 1)
    tab_ref[...] = jnp.where(lane_s == 0, i_of, jnp.where(lane_s == 1, j_of, 0.0)).astype(jnp.int32)
    w_cross = jnp.where(i_of == j_of, 0.0, w_of)
    for q in range(3 * ORB):
        coef_ref[0, q] = jnp.broadcast_to(jnp.where(i_of == q, w_of, 0.0), (slots, 128))
        coef_ref[1, q] = jnp.broadcast_to(jnp.where(j_of == q, w_cross, 0.0), (slots, 128))


def plan(slots, classes, pair_mask):
    table, same_kind, before = candidates()
    vmem = pl.BlockSpec(memory_space=pltpu.VMEM)
    return pl.pallas_call(
        functools.partial(plan_kernel, slots, classes),
        out_shape=(
            jax.ShapeDtypeStruct((slots, 128), jnp.int32),
            jax.ShapeDtypeStruct((2, 3 * ORB, slots, 128), F32),
            jax.ShapeDtypeStruct((1,), jnp.int32),
        ),
        in_specs=[vmem] * 4,
        out_specs=(vmem, vmem, pl.BlockSpec(memory_space=pltpu.SMEM)),
        name="plan",
    )(pair_mask, jnp.asarray(table), jnp.asarray(same_kind), jnp.asarray(before))


def split_sum(low_mask, tall):
    outs = []
    for t in range(tall.shape[1] // 128):
        top0, bot0, top1, bot1 = (
            tall[32 * u : 32 * (u + 1), t * 128 : (t + 1) * 128] for u in range(4)
        )
        outs.append(
            jnp.where(low_mask, top0, bot1) + pltpu.roll(jnp.where(low_mask, bot0, top1), 64, 1)
        )
    return outs


def mega_kernel(edge_slots, inner_slots, *refs):
    rounds = (max(edge_slots, inner_slots) + 3) // 4
    (tab, coef, ax_ref, wz_ref, ay_ref, ai_ref, orb_hbm, out_ref) = refs[:8]
    orbs = refs[8 : 8 + NC]
    sums = refs[8 + NC : 8 + 2 * NC]
    back = refs[8 + 2 * NC : 8 + 3 * NC]
    (rho, cube, work, vout, vrecv, ktab) = refs[8 + 3 * NC : 14 + 3 * NC]
    (lsem, z1s, z1r, x1s, x1r, x2s, x2r, z2s, z2r) = refs[14 + 3 * NC :]

    groups = lax.axis_size("band")
    band = lax.axis_index("band")
    me = lax.axis_index("grid")
    z = lax.rem(band, 4)
    on_edge = 1 - lax.rem((z + 1) // 2, 2)
    held = inner_slots + on_edge * (edge_slots - inner_slots)
    chip, core = me // 2, lax.rem(me, 2)

    def slot_of(k, r):
        return (
            4 * r
            + 2 * (core if k in (0, 2) else 1 - core)
            + (chip if k in (0, 1) else 1 - chip)
        )

    def rounds_of(k):
        return (held + 3 - slot_of(k, 0)) // 4

    left = lax.rem(band + groups - 1, groups)
    right = lax.rem(band + 1, groups)
    peers = {
        0: me,
        1: me + 1 - 2 * lax.rem(me, 2),
        2: lax.rem(me + 2, 4),
        3: 3 - me,
    }

    def local_copy(c):
        return pltpu.make_async_copy(
            orb_hbm.at[:, :, pl.ds(c * CL, CL)], orbs[c].at[pl.ds(ORB, ORB)], lsem.at[c]
        )

    for c in range(NC):
        local_copy(c).start()

    barrier = pltpu.get_barrier_semaphore()
    for target in (left, right):
        pl.semaphore_signal(barrier, inc=1, device_id=(target, me), device_id_type=MESH)
    for k in (1, 2, 3):
        pl.semaphore_signal(barrier, inc=1, device_id=(band, peers[k]), device_id_type=MESH)
    pl.semaphore_wait(barrier, 5)

    def z1(side, c):
        return pltpu.make_async_remote_copy(
            src_ref=orbs[c].at[pl.ds(ORB, ORB)],
            dst_ref=orbs[c].at[pl.ds(2 * ORB if side == 0 else 0, ORB)],
            send_sem=z1s.at[side, c],
            recv_sem=z1r.at[side, c],
            device_id=(left if side == 0 else right, me),
            device_id_type=MESH,
        )

    for c in range(NC):
        local_copy(c).wait()
        z1(0, c).start()
        z1(1, c).start()

    low_mask = lax.broadcasted_iota(jnp.int32, (32, 128), 1) < 64

    def signed(k):
        return jnp.where(k < NG // 2, k, k - NG)

    lane = lax.broadcasted_iota(jnp.int32, (32, 128), 1)
    sub = lax.broadcasted_iota(jnp.int32, (32, 128), 0)
    fy = signed(sub + jnp.where(low_mask, 0, 32))
    fz = signed(jnp.where(low_mask, lane, lane - 64))
    flat = fy * fy + fz * fz

    def fill(kx, carry):
        fx = signed(kx)
        squared = flat + fx * fx
        safe = jnp.maximum(squared, 1).astype(F32)
        ktab[pl.ds(pl.multiple_of(kx * 32, 32), 32), :] = jnp.where(
            squared > 0, (BOX * BOX / np.pi) / safe, 0.0
        )
        return carry

    lax.fori_loop(0, NG, fill, 0)

    def x1(k, r, c):
        return pltpu.make_async_remote_copy(
            src_ref=rho.at[k - 1, r, pl.ds(c * CY, CY)],
            dst_ref=cube.at[r, pl.ds(c * CY, CY), me],
            send_sem=x1s.at[k - 1, r, c],
            recv_sem=x1r.at[k - 1, r, c],
            device_id=(band, peers[k]),
            device_id_type=MESH,
        )

    def x2(k, r, c):
        return pltpu.make_async_remote_copy(
            src_ref=vout.at[r, pl.ds(c * CY, CY), peers[k]],
            dst_ref=vrecv.at[k - 1, r, pl.ds(c * CY, CY)],
            send_sem=x2s.at[k - 1, r, c],
            recv_sem=x2r.at[k - 1, r, c],
            device_id=(band, peers[k]),
            device_id_type=MESH,
        )

    def z2(side, c):
        return pltpu.make_async_remote_copy(
            src_ref=sums[c].at[pl.ds(0 if side == 0 else 2 * ORB, ORB)],
            dst_ref=back[c].at[1 if side == 0 else 0],
            send_sem=z2s.at[side, c],
            recv_sem=z2r.at[side, c],
            device_id=(left if side == 0 else right, me),
            device_id_type=MESH,
        )

    def lanes(y):
        return pl.ds(pl.multiple_of(y * 128, 128), 128)

    def densities(c, r, k):
        slot = slot_of(k, r)
        i, j = tab[slot, 0], tab[slot, 1]

        def one_tile(y, carry):
            value = orbs[c][i, :, lanes(y)] * orbs[c][j, :, lanes(y)]
            if k == 0:
                cube[r, c * CY + y, me] = value
            else:
                rho[k - 1, r, c * CY + y] = value
            return carry

        lax.fori_loop(0, CY, one_tile, 0, unroll=4)
        if k:
            x1(k, r, c).start()

    order = []
    for c in range(NC):
        order.append((c, 0))
        if c % 2 == 0:
            order.append((c // 2, 1))
    order += [(c, 1) for c in range((NC + 1) // 2, NC)]
    order += [(c, r) for r in range(2, rounds) for c in range(NC)]
    seen = set()
    for c, r in order:
        if r >= rounds:
            continue
        if c not in seen:
            seen.add(c)
            z1(0, c).wait_recv()
            z1(1, c).wait_recv()

        for k in (2, 3, 1, 0):

            @pl.when(slot_of(k, r) < held)
            def _():
                densities(c, r, k)

    ax = ax_ref[...]
    wz = wz_ref[...]

    def along_z(tiles):
        stacked = jnp.concatenate(tiles, axis=0)
        hi, lo = hi_lo(stacked)
        wide = jnp.dot(jnp.concatenate([hi, lo], axis=1), wz, preferred_element_type=F32)
        both = wide[:, :128] + wide[:, 128:]
        return [both[t * NG : (t + 1) * NG] for t in range(len(tiles))]

    def along_x(tiles):
        outs = []
        for t in range(0, len(tiles), 2):
            hi, lo = hi_lo(jnp.concatenate([tiles[t], tiles[t + 1]], axis=1))
            wide = jnp.dot(ax, jnp.concatenate([hi, hi, lo], axis=0), preferred_element_type=F32)
            outs += [wide[:, :128], wide[:, 128:]]
        return outs

    def work_rows(r, y):
        return pl.ds(pl.multiple_of((r * 32 + y) * PITCH, 8), NG)

    def forward(r, c):
        for k in (1, 2, 3):
            x1(k, r, c).wait_recv()
        tiles = [cube[r, c * CY + t].reshape(NG, 128) for t in range(CY)]
        tiles = along_z(along_x(tiles))
        for t in range(CY):
            work[work_rows(r, c * CY + t), :] = tiles[t]

    def spread(tiles):
        hi, lo = hi_lo(jnp.concatenate(tiles, axis=1))
        return jnp.concatenate([hi, hi, lo], axis=0)

    ay = ay_ref[...]
    ai = ai_ref[...]

    def middle(r, g):
        base = r * (32 * PITCH) + g * KX
        for t in range(0, KX, 2):
            tiles = [work[pl.ds(base + t + u, 32, stride=PITCH), :] for u in range(2)]
            tiles = split_sum(low_mask, jnp.dot(ay, spread(tiles), preferred_element_type=F32))
            tiles = [
                tiles[u] * ktab[pl.ds(pl.multiple_of((g * KX + t + u) * 32, 32), 32), :]
                for u in range(2)
            ]
            tiles = split_sum(low_mask, jnp.dot(ai, spread(tiles), preferred_element_type=F32))
            for u in range(2):
                work[pl.ds(base + t + u, 32, stride=PITCH), :] = tiles[u]

    def inverse(r, c):
        tiles = [work[work_rows(r, c * CY + t), :] for t in range(CY)]
        tiles = along_x(along_z(tiles))
        for t in range(CY):
            vout[r, c * CY + t] = tiles[t].reshape(4, 16, 128)

    def return_chunk(r, c):
        for k in (2, 3, 1):
            x2(k, r, c).start()

    def looped(count, step):
        def body(i, carry):
            step(i)
            return carry

        lax.fori_loop(0, count, body, 0)

    @functools.partial(looped, rounds_of(0))
    def _(r):
        looped(NC, functools.partial(forward, r))
        looped(NG // KX, functools.partial(middle, r))

        @functools.partial(looped, NC)
        def _(c):
            inverse(r, c)

            @pl.when((c < EARLY) | (r == rounds_of(0) - 1))
            def _():
                return_chunk(r, c)

            @pl.when((c >= EARLY) & (r == rounds_of(0) - 1))
            def _():
                looped(r, lambda before: return_chunk(before, c))

    for c in range(NC):
        sums[c][...] = jnp.zeros_like(sums[c])

    def accumulate(c, r, k):
        slot = slot_of(k, r)
        i, j = tab[slot, 0], tab[slot, 1]
        if k:
            x2(k, r, c).wait_recv()

        @functools.partial(looped, CY)
        def _(y):
            if k == 0:
                v = vout[r, c * CY + y, me]
            else:
                v = vrecv[k - 1, r, c * CY + y]
            on_i = v * orbs[c][j, :, lanes(y)]
            on_j = v * orbs[c][i, :, lanes(y)]
            for q in range(3 * ORB):
                sums[c][q, :, lanes(y)] += (
                    coef[0, q, pl.ds(slot, 1), :] * on_i + coef[1, q, pl.ds(slot, 1), :] * on_j
                )

    def both(c, r):
        for k in (0, 1, 2, 3):

            @pl.when(slot_of(k, r) < held)
            def _():
                accumulate(c, r, k)

    last = (held + 3) // 4 - 1

    @functools.partial(looped, last)
    def _(r):
        for c in range(EARLY):
            both(c, r)

    for c in range(NC):
        if c >= EARLY:
            looped(last, functools.partial(both, c))
        both(c, last)
        z2(0, c).start()
        z2(1, c).start()

    for c in range(NC):
        z2(0, c).wait_recv()
        z2(1, c).wait_recv()
        for a in range(ORB):
            out_ref[a, :, pl.ds(c * CL, CL)] = -MIXING * (
                sums[c][ORB + a] + (back[c][0, a] + back[c][1, a])
            )

    for c in range(NC):
        for side in range(2):
            z1(side, c).wait_send()
            z2(side, c).wait_send()

    for k in (1, 2, 3):

        @functools.partial(looped, rounds_of(k))
        def _(r):
            for c in range(NC):
                x1(k, r, c).wait_send()

    @functools.partial(looped, rounds_of(0))
    def _(r):
        for c in range(NC):
            for k in (1, 2, 3):
                x2(k, r, c).wait_send()


def mega(slots, collective_id, tab, coef, orbitals):
    rounds = (max(slots) + 3) // 4
    ax, wz, ay, ai = tables()
    vmem = pl.BlockSpec(memory_space=pltpu.VMEM)
    planes = orbitals.shape[1]
    dma = pltpu.SemaphoreType.DMA
    return pl.pallas_call(
        functools.partial(mega_kernel, *slots),
        out_shape=jax.ShapeDtypeStruct(orbitals.shape, F32),
        in_specs=[pl.BlockSpec(memory_space=pltpu.SMEM)]
        + [vmem] * 5
        + [pl.BlockSpec(memory_space=pl.ANY)],
        out_specs=vmem,
        scratch_shapes=[pltpu.VMEM((3 * ORB, planes, CL), F32) for _ in range(2 * NC)]
        + [pltpu.VMEM((2, ORB, planes, CL), F32) for _ in range(NC)]
        + [
            pltpu.VMEM((3, rounds, 32, planes, 128), F32),
            pltpu.VMEM((rounds, 32, 4, planes, 128), F32),
            pltpu.VMEM((rounds * 32 * PITCH, 128), F32),
            pltpu.VMEM((rounds, 32, 4, planes, 128), F32),
            pltpu.VMEM((3, rounds, 32, planes, 128), F32),
            pltpu.VMEM((NG * 32, 128), F32),
            dma((NC,)),
            dma((2, NC)),
            dma((2, NC)),
            dma((3, rounds, NC)),
            dma((3, rounds, NC)),
            dma((3, rounds, NC)),
            dma((3, rounds, NC)),
            dma((2, NC)),
            dma((2, NC)),
        ],
        compiler_params=pltpu.CompilerParams(
            collective_id=collective_id, has_side_effects=True, vmem_limit_bytes=56 * 1024 * 1024
        ),
        name="mega%d_%d" % slots,
    )(
        tab,
        coef,
        jnp.asarray(ax),
        jnp.asarray(wz),
        jnp.asarray(ay),
        jnp.asarray(ai),
        orbitals,
    )


def local(orbitals, pair_mask):
    tab, coef, index = plan(16, CLASSES, pair_mask)
    branches = [functools.partial(mega, slots, 3 + n) for n, slots in enumerate(CLASSES)]
    if len(branches) == 1:
        return branches[0](tab, coef, orbitals)
    return lax.switch(index[0], branches, tab, coef, orbitals)


def solution(mesh):
    return jax.shard_map(
        local,
        mesh=mesh,
        in_specs=(P("band", "grid", None), P()),
        out_specs=P("band", "grid", None),
        check_vma=False,
    )
```

```python
import functools

import jax
import jax.numpy as jnp
import numpy as np
from jax import lax
from jax.experimental import pallas as pl
from jax.experimental.pallas import tpu as pltpu
from jax.sharding import PartitionSpec as P

NG = 64
ORB = 3
MIXING = 0.25
BOX = 16.0
NC = 4
CY = 32 // NC
CL = CY * 128
EARLY = NC // 2
KX = 16
CLASSES = ((6, 10), (7, 11), (8, 12), (9, 12), (12, 12))
PITCH = 72
MESH = pl.DeviceIdType.MESH
F32 = jnp.float32
BF16 = jnp.bfloat16


def hi_lo(values):
    hi = values.astype(BF16)
    return hi, (values - hi.astype(F32)).astype(BF16)


def host_hi_lo(values):
    hi = values.astype(np.float32).astype(BF16)
    return hi, (values - hi.astype(np.float64)).astype(np.float32).astype(BF16)


def tables():
    n = np.arange(NG)
    angle = 2.0 * np.pi * ((n[:, None] * n[None, :]) % NG) / NG
    h = (np.cos(angle) + np.sin(angle)) / 8.0
    hh, hl = host_hi_lo(h)
    ax = np.concatenate([hh, hl, hh], axis=1)
    bh, bl = host_hi_lo(np.kron(np.eye(2), h))
    wz = np.block([[bh, bl], [bh, np.zeros_like(bl)]])
    fh, fl = host_hi_lo(np.concatenate([h[:, 0::2], h[:, 1::2]], axis=0))
    ay = np.concatenate([fh, fl, fh], axis=1)
    back = np.concatenate([h[0::2], h[1::2]], axis=0)
    gh, gl = host_hi_lo(np.concatenate([back[:, :32], back[:, 32:]], axis=0))
    ai = np.concatenate([gh, gl, gh], axis=1)
    return ax, wz, ay, ai


def candidates():
    rows = []
    for first, second, same, kind in (
        (0, 2, False, 0),
        (1, 2, False, 1),
        (0, 1, False, 2),
        (1, 1, True, 3),
        (0, 0, True, 4),
        (2, 2, True, 5),
    ):
        for a in range(ORB):
            for b in range(ORB):
                if not same or a <= b:
                    rows.append((first, a, second, b, kind, 1))
    table = np.zeros((8, 128), np.int32)
    for c, row in enumerate(rows):
        table[:6, c] = row
    kind = np.where(table[5] > 0, table[4], -1)
    before = np.arange(128)[:, None] < np.arange(128)[None, :]
    same_kind = before & (kind[:, None] == kind[None, :])
    return table, same_kind.astype(np.float32), before.astype(np.float32)


def plan_kernel(slots, classes, mask_ref, cand_ref, same_ref, before_ref, tab_ref, coef_ref, class_ref):
    norb = mask_ref.shape[0]
    groups = norb // ORB
    group = lax.axis_index("band")
    m = mask_ref[...].astype(F32)
    rows = lax.broadcasted_iota(jnp.int32, (norb, norb), 0)
    cols = lax.broadcasted_iota(jnp.int32, (norb, norb), 1)
    brow = (rows * 21846) >> 16
    bcol = (cols * 21846) >> 16
    sep = jnp.where(bcol >= brow, bcol - brow, bcol - brow + groups)

    def row_sum(keep):
        return jnp.sum(jnp.where(keep, m, 0.0), axis=1, keepdims=True)

    r0 = row_sum((sep == 0) & (rows <= cols))
    r1 = row_sum(sep == 1)
    r2 = row_sum(sep == 2)
    gb = (lax.broadcasted_iota(jnp.int32, (norb, 128), 0) * 21846) >> 16
    lane = lax.broadcasted_iota(jnp.int32, (norb, 128), 1)
    nxt = jnp.where(gb == groups - 1, 0, gb + 1)
    prv = jnp.where(gb == 0, groups - 1, gb - 1)

    def to_lanes(values, place):
        return jnp.sum(jnp.where(place == lane, values, 0.0), axis=0, keepdims=True)

    n0 = to_lanes(r0, gb)
    n0_next = to_lanes(r0, prv)
    n1 = to_lanes(r1, gb)
    n2_prev = to_lanes(r2, nxt)
    load = n2_prev + n1 + n0
    sub = lax.broadcasted_iota(jnp.int32, (128, 128), 0)
    lan = lax.broadcasted_iota(jnp.int32, (128, 128), 1)
    sub1 = lax.broadcasted_iota(jnp.int32, (128, 1), 0)
    lan1 = lax.broadcasted_iota(jnp.int32, (1, 128), 1)
    eye = sub == lan

    def to_rows(values):
        return jnp.sum(jnp.where(eye, values, 0.0), axis=1, keepdims=True)

    low = -n0_next
    high = to_rows(n1 + n0)
    prev_rows = to_rows(n2_prev)
    load_rows = jnp.where(sub < groups, to_rows(load), 0.0)
    prefix = jnp.sum(jnp.where(sub <= lan, load_rows, 0.0), axis=0, keepdims=True)
    total = jnp.sum(load_rows, axis=0, keepdims=True)
    path = to_rows(prefix) - prefix + jnp.where(sub < lan, total, 0.0) + low
    path = jnp.where(lan < groups, path, -1e9)

    def edges_to(m):
        return 2 * (m // 4) + 1 + lax.rem(m, 4) // 3

    def held_to(m, edge, inner):
        return (inner * (m + 1) + (edge - inner) * edges_to(m)).astype(F32)

    is_edge = lax.rem((lax.rem(sub1, 4) + 1) // 2, 2) == 0
    choice, flow = None, None
    for index in reversed(range(len(classes))):
        edge, inner = classes[index]
        held = float((edge + inner) * (groups // 2))
        need = path - held_to(sub1, edge, inner) + held_to(lan1, edge, inner)
        need = jnp.max(jnp.where(sub < lan, need - held, need), axis=1, keepdims=True)
        if choice is None:
            choice, flow = jnp.full((1, 1), float(index), F32), need
        else:
            over = jnp.maximum(need - high, prev_rows - jnp.where(is_edge, float(edge), float(inner)))
            over = jnp.where(sub1 < groups, over, -1e9)
            worst = jnp.maximum(jnp.max(over, axis=0, keepdims=True), total[:, :1] - held)
            fits = worst < 0.5
            choice = jnp.where(fits, float(index), choice)
            flow = jnp.where(fits, need, flow)
    class_ref[0] = jnp.max(choice).astype(jnp.int32)

    left = jnp.where(group == 0, groups - 1, group - 1)
    right = jnp.where(group == groups - 1, 0, group + 1)

    def at_row(values, index):
        return jnp.sum(jnp.where(sub1 == index, values, 0.0), axis=0, keepdims=True)

    def at_lane(values, index):
        return jnp.sum(jnp.where(lan1 == index, values, 0.0), axis=1, keepdims=True)

    f_here, f_left = at_row(flow, group), at_row(flow, left)
    n1_here, n1_left = at_lane(n1, group), at_lane(n1, left)
    n0_here, n0_right = at_lane(n0, group), at_lane(n0, right)

    cand = cand_ref[...]

    def orbital_of(block, inner):
        b = group + block - 1
        b = jnp.where(b < 0, b + groups, jnp.where(b >= groups, b - groups, b))
        return b * ORB + inner

    row_id = orbital_of(cand[0:1], cand[1:2])
    col_id = orbital_of(cand[2:3], cand[3:4])
    kind = cand[4:5]
    valid = cand[5:6] > 0
    orb = lax.broadcasted_iota(jnp.int32, (norb, 128), 0)
    col_hot = (orb == col_id).astype(F32)
    picked = jnp.dot(m, col_hot, preferred_element_type=F32)
    live = jnp.sum(jnp.where(orb == row_id, picked, 0.0), axis=0, keepdims=True)
    live = jnp.where(valid, live, 0.0)
    rank = jnp.dot(
        jnp.broadcast_to(live, (8, 128)), same_ref[...], preferred_element_type=F32
    )[0:1]
    big = 1e9
    x1 = jnp.minimum(jnp.maximum(f_here, 0.0), n1_here)
    y1 = jnp.minimum(jnp.maximum(f_left, 0.0), n1_left)
    b0 = jnp.maximum(f_here - n1_here, 0.0)
    a0 = jnp.maximum(-f_left, 0.0)
    low_rank = jnp.where(
        kind == 1,
        x1,
        jnp.where(kind == 3, b0, jnp.where(kind == 5, n0_right - jnp.maximum(-f_here, 0.0), 0.0)),
    )
    high_rank = jnp.where(
        kind == 2,
        y1,
        jnp.where(
            kind == 3, n0_here - a0, jnp.where(kind == 4, jnp.maximum(f_left - n1_left, 0.0), big)
        ),
    )
    active = jnp.where((rank >= low_rank) & (rank < high_rank), live, 0.0)
    place = jnp.dot(
        jnp.broadcast_to(active, (8, 128)), before_ref[...], preferred_element_type=F32
    )[0:1]
    slot = lax.broadcasted_iota(jnp.int32, (slots, 128), 0).astype(F32)
    hot = jnp.where(place == slot, active, 0.0)
    first = (cand[0:1] * ORB + cand[1:2]).astype(F32)
    second = (cand[2:3] * ORB + cand[3:4]).astype(F32)
    i_of = jnp.sum(hot * first, axis=1, keepdims=True)
    j_of = jnp.sum(hot * second, axis=1, keepdims=True)
    w_of = jnp.sum(hot, axis=1, keepdims=True)
    lane_s = lax.broadcasted_iota(jnp.int32, (slots, 128), 1)
    tab_ref[...] = jnp.where(lane_s == 0, i_of, jnp.where(lane_s == 1, j_of, 0.0)).astype(jnp.int32)
    w_cross = jnp.where(i_of == j_of, 0.0, w_of)
    for q in range(3 * ORB):
        coef_ref[0, q] = jnp.broadcast_to(jnp.where(i_of == q, w_of, 0.0), (slots, 128))
        coef_ref[1, q] = jnp.broadcast_to(jnp.where(j_of == q, w_cross, 0.0), (slots, 128))


def plan(slots, classes, pair_mask):
    table, same_kind, before = candidates()
    vmem = pl.BlockSpec(memory_space=pltpu.VMEM)
    return pl.pallas_call(
        functools.partial(plan_kernel, slots, classes),
        out_shape=(
            jax.ShapeDtypeStruct((slots, 128), jnp.int32),
            jax.ShapeDtypeStruct((2, 3 * ORB, slots, 128), F32),
            jax.ShapeDtypeStruct((1,), jnp.int32),
        ),
        in_specs=[vmem] * 4,
        out_specs=(vmem, vmem, pl.BlockSpec(memory_space=pltpu.SMEM)),
        name="plan",
    )(pair_mask, jnp.asarray(table), jnp.asarray(same_kind), jnp.asarray(before))


def split_sum(low_mask, tall):
    outs = []
    for t in range(tall.shape[1] // 128):
        top0, bot0, top1, bot1 = (
            tall[32 * u : 32 * (u + 1), t * 128 : (t + 1) * 128] for u in range(4)
        )
        outs.append(
            jnp.where(low_mask, top0, bot1) + pltpu.roll(jnp.where(low_mask, bot0, top1), 64, 1)
        )
    return outs


def mega_kernel(edge_slots, inner_slots, *refs):
    rounds = (max(edge_slots, inner_slots) + 3) // 4
    (tab, coef, ax_ref, wz_ref, ay_ref, ai_ref, orb_hbm, out_ref) = refs[:8]
    orbs = refs[8 : 8 + NC]
    sums = refs[8 + NC : 8 + 2 * NC]
    back = refs[8 + 2 * NC : 8 + 3 * NC]
    (rho, cube, work, vout, vrecv, ktab) = refs[8 + 3 * NC : 14 + 3 * NC]
    (lsem, z1s, z1r, x1s, x1r, x2s, x2r, z2s, z2r) = refs[14 + 3 * NC :]

    groups = lax.axis_size("band")
    band = lax.axis_index("band")
    me = lax.axis_index("grid")
    z = lax.rem(band, 4)
    on_edge = 1 - lax.rem((z + 1) // 2, 2)
    held = inner_slots + on_edge * (edge_slots - inner_slots)
    chip, core = me // 2, lax.rem(me, 2)

    def slot_of(k, r):
        return (
            4 * r
            + 2 * (core if k in (0, 2) else 1 - core)
            + (chip if k in (0, 1) else 1 - chip)
        )

    def rounds_of(k):
        return (held + 3 - slot_of(k, 0)) // 4

    left = lax.rem(band + groups - 1, groups)
    right = lax.rem(band + 1, groups)
    peers = {
        0: me,
        1: me + 1 - 2 * lax.rem(me, 2),
        2: lax.rem(me + 2, 4),
        3: 3 - me,
    }

    def local_copy(c):
        return pltpu.make_async_copy(
            orb_hbm.at[:, :, pl.ds(c * CL, CL)], orbs[c].at[pl.ds(ORB, ORB)], lsem.at[c]
        )

    for c in range(NC):
        local_copy(c).start()

    barrier = pltpu.get_barrier_semaphore()
    for target in (left, right):
        pl.semaphore_signal(barrier, inc=1, device_id=(target, me), device_id_type=MESH)
    for k in (1, 2, 3):
        pl.semaphore_signal(barrier, inc=1, device_id=(band, peers[k]), device_id_type=MESH)
    pl.semaphore_wait(barrier, 5)

    def z1(side, c):
        return pltpu.make_async_remote_copy(
            src_ref=orbs[c].at[pl.ds(ORB, ORB)],
            dst_ref=orbs[c].at[pl.ds(2 * ORB if side == 0 else 0, ORB)],
            send_sem=z1s.at[side, c],
            recv_sem=z1r.at[side, c],
            device_id=(left if side == 0 else right, me),
            device_id_type=MESH,
        )

    for c in range(NC):
        local_copy(c).wait()
        z1(0, c).start()
        z1(1, c).start()

    low_mask = lax.broadcasted_iota(jnp.int32, (32, 128), 1) < 64

    def signed(k):
        return jnp.where(k < NG // 2, k, k - NG)

    lane = lax.broadcasted_iota(jnp.int32, (32, 128), 1)
    sub = lax.broadcasted_iota(jnp.int32, (32, 128), 0)
    fy = signed(sub + jnp.where(low_mask, 0, 32))
    fz = signed(jnp.where(low_mask, lane, lane - 64))
    flat = fy * fy + fz * fz

    def fill(kx, carry):
        fx = signed(kx)
        squared = flat + fx * fx
        safe = jnp.maximum(squared, 1).astype(F32)
        ktab[pl.ds(pl.multiple_of(kx * 32, 32), 32), :] = jnp.where(
            squared > 0, (BOX * BOX / np.pi) / safe, 0.0
        )
        return carry

    lax.fori_loop(0, NG, fill, 0)

    def x1(k, r, c):
        return pltpu.make_async_remote_copy(
            src_ref=rho.at[k - 1, r, pl.ds(c * CY, CY)],
            dst_ref=cube.at[r, pl.ds(c * CY, CY), me],
            send_sem=x1s.at[k - 1, r, c],
            recv_sem=x1r.at[k - 1, r, c],
            device_id=(band, peers[k]),
            device_id_type=MESH,
        )

    def x2(k, r, c):
        return pltpu.make_async_remote_copy(
            src_ref=vout.at[r, pl.ds(c * CY, CY), peers[k]],
            dst_ref=vrecv.at[k - 1, r, pl.ds(c * CY, CY)],
            send_sem=x2s.at[k - 1, r, c],
            recv_sem=x2r.at[k - 1, r, c],
            device_id=(band, peers[k]),
            device_id_type=MESH,
        )

    def z2(side, c):
        return pltpu.make_async_remote_copy(
            src_ref=sums[c].at[pl.ds(0 if side == 0 else 2 * ORB, ORB)],
            dst_ref=back[c].at[1 if side == 0 else 0],
            send_sem=z2s.at[side, c],
            recv_sem=z2r.at[side, c],
            device_id=(left if side == 0 else right, me),
            device_id_type=MESH,
        )

    def lanes(y):
        return pl.ds(pl.multiple_of(y * 128, 128), 128)

    def densities(c, r, k):
        slot = slot_of(k, r)
        i, j = tab[slot, 0], tab[slot, 1]

        def one_tile(y, carry):
            value = orbs[c][i, :, lanes(y)] * orbs[c][j, :, lanes(y)]
            if k == 0:
                cube[r, c * CY + y, me] = value
            else:
                rho[k - 1, r, c * CY + y] = value
            return carry

        lax.fori_loop(0, CY, one_tile, 0, unroll=4)
        if k:
            x1(k, r, c).start()

    order = []
    for c in range(NC):
        order.append((c, 0, True, True))
        if c % 2 == 0:
            order.append((c // 2, 1, False, True))
    order += [(c, 1, True, c >= (NC + 1) // 2) for c in range(NC)]
    order += [(c, r, True, True) for r in range(2, rounds) for c in range(NC)]
    seen = set()
    for c, r, at_edge, at_inner in order:
        if r >= rounds:
            continue
        if c not in seen:
            seen.add(c)
            z1(0, c).wait_recv()
            z1(1, c).wait_recv()
        for k in (2, 3, 1, 0):
            here = slot_of(k, r) < held
            if not (at_edge and at_inner):
                here &= on_edge == (1 if at_edge else 0)

            @pl.when(here)
            def _():
                densities(c, r, k)

    ax = ax_ref[...]
    wz = wz_ref[...]

    def along_z(tiles):
        stacked = jnp.concatenate(tiles, axis=0)
        hi, lo = hi_lo(stacked)
        wide = jnp.dot(jnp.concatenate([hi, lo], axis=1), wz, preferred_element_type=F32)
        both = wide[:, :128] + wide[:, 128:]
        return [both[t * NG : (t + 1) * NG] for t in range(len(tiles))]

    def along_x(tiles):
        outs = []
        for t in range(0, len(tiles), 2):
            hi, lo = hi_lo(jnp.concatenate([tiles[t], tiles[t + 1]], axis=1))
            wide = jnp.dot(ax, jnp.concatenate([hi, hi, lo], axis=0), preferred_element_type=F32)
            outs += [wide[:, :128], wide[:, 128:]]
        return outs

    def work_rows(r, y):
        return pl.ds(pl.multiple_of((r * 32 + y) * PITCH, 8), NG)

    def forward(r, c):
        for k in (1, 2, 3):
            x1(k, r, c).wait_recv()
        tiles = [cube[r, c * CY + t].reshape(NG, 128) for t in range(CY)]
        tiles = along_z(along_x(tiles))
        for t in range(CY):
            work[work_rows(r, c * CY + t), :] = tiles[t]

    def spread(tiles):
        hi, lo = hi_lo(jnp.concatenate(tiles, axis=1))
        return jnp.concatenate([hi, hi, lo], axis=0)

    ay = ay_ref[...]
    ai = ai_ref[...]

    def middle(r, g):
        base = r * (32 * PITCH) + g * KX
        for t in range(0, KX, 2):
            tiles = [work[pl.ds(base + t + u, 32, stride=PITCH), :] for u in range(2)]
            tiles = split_sum(low_mask, jnp.dot(ay, spread(tiles), preferred_element_type=F32))
            tiles = [
                tiles[u] * ktab[pl.ds(pl.multiple_of((g * KX + t + u) * 32, 32), 32), :]
                for u in range(2)
            ]
            tiles = split_sum(low_mask, jnp.dot(ai, spread(tiles), preferred_element_type=F32))
            for u in range(2):
                work[pl.ds(base + t + u, 32, stride=PITCH), :] = tiles[u]

    def inverse(r, c):
        tiles = [work[work_rows(r, c * CY + t), :] for t in range(CY)]
        tiles = along_x(along_z(tiles))
        for t in range(CY):
            vout[r, c * CY + t] = tiles[t].reshape(4, 16, 128)

    def return_chunk(r, c):
        for k in (2, 3, 1):
            x2(k, r, c).start()

    def looped(count, step):
        def body(i, carry):
            step(i)
            return carry

        lax.fori_loop(0, count, body, 0)

    @functools.partial(looped, rounds_of(0))
    def _(r):
        looped(NC, functools.partial(forward, r))
        looped(NG // KX, functools.partial(middle, r))

        @functools.partial(looped, NC)
        def _(c):
            inverse(r, c)

            @pl.when((r < on_edge) | (c < EARLY) | (r == rounds_of(0) - 1))
            def _():
                return_chunk(r, c)

            @pl.when((c >= EARLY) & (r == rounds_of(0) - 1))
            def _():
                looped(r - on_edge, lambda n: return_chunk(n + on_edge, c))

    for c in range(NC):
        sums[c][...] = jnp.zeros_like(sums[c])

    def accumulate(c, r, k):
        slot = slot_of(k, r)
        i, j = tab[slot, 0], tab[slot, 1]
        if k:
            x2(k, r, c).wait_recv()

        @functools.partial(looped, CY)
        def _(y):
            if k == 0:
                v = vout[r, c * CY + y, me]
            else:
                v = vrecv[k - 1, r, c * CY + y]
            on_i = v * orbs[c][j, :, lanes(y)]
            on_j = v * orbs[c][i, :, lanes(y)]
            for q in range(3 * ORB):
                sums[c][q, :, lanes(y)] += (
                    coef[0, q, pl.ds(slot, 1), :] * on_i + coef[1, q, pl.ds(slot, 1), :] * on_j
                )

    def both(c, r):
        for k in (0, 1, 2, 3):

            @pl.when(slot_of(k, r) < held)
            def _():
                accumulate(c, r, k)

    last = (held + 3) // 4 - 1

    @functools.partial(looped, last)
    def _(r):
        for c in range(EARLY):
            both(c, r)

    for c in range(NC):
        if c >= EARLY:
            looped(last, functools.partial(both, c))
        both(c, last)
        z2(0, c).start()
        z2(1, c).start()

    for c in range(NC):
        z2(0, c).wait_recv()
        z2(1, c).wait_recv()
        for a in range(ORB):
            out_ref[a, :, pl.ds(c * CL, CL)] = -MIXING * (
                sums[c][ORB + a] + (back[c][0, a] + back[c][1, a])
            )

    for c in range(NC):
        for side in range(2):
            z1(side, c).wait_send()
            z2(side, c).wait_send()

    for k in (1, 2, 3):

        @functools.partial(looped, rounds_of(k))
        def _(r):
            for c in range(NC):
                x1(k, r, c).wait_send()

    @functools.partial(looped, rounds_of(0))
    def _(r):
        for c in range(NC):
            for k in (1, 2, 3):
                x2(k, r, c).wait_send()


def mega(slots, collective_id, tab, coef, orbitals):
    rounds = (max(slots) + 3) // 4
    ax, wz, ay, ai = tables()
    vmem = pl.BlockSpec(memory_space=pltpu.VMEM)
    planes = orbitals.shape[1]
    dma = pltpu.SemaphoreType.DMA
    return pl.pallas_call(
        functools.partial(mega_kernel, *slots),
        out_shape=jax.ShapeDtypeStruct(orbitals.shape, F32),
        in_specs=[pl.BlockSpec(memory_space=pltpu.SMEM)]
        + [vmem] * 5
        + [pl.BlockSpec(memory_space=pl.ANY)],
        out_specs=vmem,
        scratch_shapes=[pltpu.VMEM((3 * ORB, planes, CL), F32) for _ in range(2 * NC)]
        + [pltpu.VMEM((2, ORB, planes, CL), F32) for _ in range(NC)]
        + [
            pltpu.VMEM((3, rounds, 32, planes, 128), F32),
            pltpu.VMEM((rounds, 32, 4, planes, 128), F32),
            pltpu.VMEM((rounds * 32 * PITCH, 128), F32),
            pltpu.VMEM((rounds, 32, 4, planes, 128), F32),
            pltpu.VMEM((3, rounds, 32, planes, 128), F32),
            pltpu.VMEM((NG * 32, 128), F32),
            dma((NC,)),
            dma((2, NC)),
            dma((2, NC)),
            dma((3, rounds, NC)),
            dma((3, rounds, NC)),
            dma((3, rounds, NC)),
            dma((3, rounds, NC)),
            dma((2, NC)),
            dma((2, NC)),
        ],
        compiler_params=pltpu.CompilerParams(
            collective_id=collective_id, has_side_effects=True, vmem_limit_bytes=56 * 1024 * 1024
        ),
        name="mega%d_%d" % slots,
    )(
        tab,
        coef,
        jnp.asarray(ax),
        jnp.asarray(wz),
        jnp.asarray(ay),
        jnp.asarray(ai),
        orbitals,
    )


def local(orbitals, pair_mask):
    tab, coef, index = plan(16, CLASSES, pair_mask)
    branches = [functools.partial(mega, slots, 3 + n) for n, slots in enumerate(CLASSES)]
    if len(branches) == 1:
        return branches[0](tab, coef, orbitals)
    return lax.switch(index[0], branches, tab, coef, orbitals)


def solution(mesh):
    return jax.shard_map(
        local,
        mesh=mesh,
        in_specs=(P("band", "grid", None), P()),
        out_specs=P("band", "grid", None),
        check_vma=False,
    )
```
